256 devices in a mesh: pop: 64 (over x, z, core), mp: 4 (over y).
Axes of the slice: x: 4, y: 4, z: 8, core: 2. Of those that a mesh axis runs over, the one named last changes fastest.
Arguments:
- tokens: bfloat16 [256, 3584], replicated, may hold values from -60 to 60
- target: bfloat16 [256, 3584], P(None, 'mp'), may hold values from -6 to 6
- w_query: bfloat16 [3584, 3584], P('pop', 'mp'), may hold values from -0.09375 to 0.09375
- w_key: bfloat16 [3584, 512], P(None, 'mp'), may hold values from -0.09375 to 0.09375
- w_value: bfloat16 [3584, 512], P(None, 'mp'), may hold values from -0.09375 to 0.09375
- w_out: bfloat16 [3584, 3584], P('mp', 'pop'), may hold values from -0.09375 to 0.09375
- query_left_factors: bfloat16 [64, 3584, 4], P('pop'), may hold values from -0.09375 to 0.09375
- query_right_factors: bfloat16 [64, 4, 3584], P('pop', None, 'mp'), may hold values from -6 to 6
- o_left: bfloat16 [64, 3584, 4], P('pop', 'mp'), may hold values from -0.09375 to 0.09375
- o_right: bfloat16 [64, 4, 3584], P('pop'), may hold values from -6 to 6
- member_ids: int32 [64], P('pop'), may hold values from 0 to 63, each once
Outputs:
- grad_query: float32 [3584, 3584], P('pop', 'mp')
- grad_out: float32 [3584, 3584], P('mp', 'pop')
- fitness: float32 [64], P('pop')
The draws below stay inside these ranges and needn't reach their ends.
Inputs may be any that keep to these rules, and one draw needn't show every extreme that they name: `member_ids`: every number from 0 to 63 appears once.
All inputs are finite; a program needn't handle non-finite values.
Results may differ from the reference program's by a relative error of at most 0.005.
Values may be sent and summed in bfloat16 or wider, within the bound.
A program may use at most 64 MiB of HBM per device.

```python
import math
import jax
import jax.numpy as jnp
from jax import lax

D = 3584
HEADS = 28
KV_HEADS = 4
HEAD_DIM = 128
RANK = 4
TOK = 256
F = 3584
KVF = 512
M = 64
N_MP = 4


def draw_tokens(key, part):
    first = jax.random.fold_in(key, 0)
    normal = jax.random.normal(first, (TOK, D), jnp.float32)
    return jnp.clip(normal, -5.0, 5.0).astype(jnp.bfloat16)


def level_of(stream_key, dims, cuts, low, largest):
    def one(axis_at, parts):
        draws = jax.random.uniform(jax.random.fold_in(jax.random.fold_in(stream_key, 6), axis_at), (parts,), jnp.float32, low / len(cuts), largest / len(cuts))
        return jnp.repeat(jnp.exp(draws), dims[axis_at] // parts).reshape((-1,) + (1,) * (len(dims) - axis_at - 1))

    gain = one(*cuts[0])
    for cut in cuts[1:]:
        gain = gain * one(*cut)
    return gain


def normal_values(stream_key, shape, scale, bound, shards=(), held_as=jnp.bfloat16):
    result = scale * jax.random.normal(stream_key, shape, jnp.float32)
    if shards:
        result = result * level_of(stream_key, shape, shards, -0.22, 0.18)
    return jnp.clip(result, -bound, bound).astype(held_as)


def setup_inputs(seed: int = 0) -> dict:
    key_list = jax.random.split(jax.random.key(seed), 12)
    return {
        "tokens": draw_tokens(jax.random.fold_in(key_list[11], 71), 0),
        "target": normal_values(key_list[1], (TOK, D), 1.0, 6.0, ((1, 4),)),
        "w_query": normal_values(key_list[2], (D, F), D ** -0.5, 0.09375, ((0, 64), (1, 4))),
        "w_key": normal_values(key_list[3], (D, KVF), D ** -0.5, 0.09375, ((1, 4),)),
        "w_value": normal_values(key_list[4], (D, KVF), D ** -0.5, 0.09375, ((1, 4),)),
        "w_out": normal_values(key_list[5], (F, D), F ** -0.5, 0.09375, ((0, 4), (1, 64))),
        "query_left_factors": normal_values(key_list[6], (M, D, RANK), D ** -0.5, 0.09375, ((0, 64),)),
        "query_right_factors": normal_values(key_list[7], (M, RANK, F), 1.0, 6.0, ((0, 64), (2, 4))),
        "o_left": normal_values(key_list[8], (M, F, RANK), F ** -0.5, 0.09375, ((0, 64), (1, 4))),
        "o_right": normal_values(key_list[9], (M, RANK, D), 1.0, 6.0, ((0, 64),)),
        "member_ids": jax.random.permutation(key_list[10], M).astype(jnp.int32),
    }


noise_scale = 0.5
rope_base = 1000000.0
spread_floor = 0.001

def tables(count, head_size):
    position = jnp.arange(count, dtype=jnp.float32)
    index = jnp.arange(head_size // 2, dtype=jnp.float32)
    freq = jnp.exp(-math.log(rope_base) * 2.0 * index / head_size)
    angle = position[:, None] * freq[None, :]
    return (jnp.cos(angle)[:, None, :], jnp.sin(angle)[:, None, :])

def rotate(field, cosine_table, sine):
    half = field.shape[-1] // 2
    first = field[..., :half]
    second = field[..., half:]
    return jnp.concatenate([first * cosine_table - second * sine, second * cosine_table + first * sine], axis=-1)

def reference(tokens, target, w_query, w_key, w_value, w_out, query_left_factors, query_right_factors, o_left, o_right, member_ids):
    tok = tokens.shape[0]
    width = tokens.shape[1]
    hidden = w_query.shape[1]
    members = query_left_factors.shape[0]
    group = HEADS // KV_HEADS
    block = hidden // N_MP
    scale = HEAD_DIM ** (-0.5)
    cosine_table, sine = tables(tok, HEAD_DIM)
    base = jnp.dot(tokens, w_query, preferred_element_type=jnp.float32)
    keys = rotate(jnp.dot(tokens, w_key, preferred_element_type=jnp.float32).reshape(tok, KV_HEADS, HEAD_DIM), cosine_table, sine).astype(jnp.bfloat16)
    values = jnp.dot(tokens, w_value, preferred_element_type=jnp.float32).astype(jnp.bfloat16).reshape(tok, KV_HEADS, HEAD_DIM)
    signs = (1 - 2 * (member_ids % 2)).astype(jnp.float32)
    causal = jnp.arange(tok)[:, None] >= jnp.arange(tok)[None, :]
    target_f = target.astype(jnp.float32)

    def score(index):
        sign = signs[index]
        lowrank_product = jnp.dot(tokens, query_left_factors[index], preferred_element_type=jnp.float32).astype(jnp.bfloat16)
        query = base + noise_scale * sign * jnp.dot(lowrank_product, query_right_factors[index], preferred_element_type=jnp.float32)
        query = rotate(query.reshape(tok, HEADS, HEAD_DIM), cosine_table, sine).astype(jnp.bfloat16)
        query = query.reshape(tok, KV_HEADS, group, HEAD_DIM)
        scores = jnp.einsum('tkgd,skd->kgts', query.astype(jnp.float32), keys.astype(jnp.float32)) * scale
        scores = jnp.where(causal, scores, -1e+30)
        probs = jax.nn.softmax(scores, axis=-1).astype(jnp.bfloat16)
        mixed = jnp.einsum('kgts,skd->tkgd', probs.astype(jnp.float32), values.astype(jnp.float32)).astype(jnp.bfloat16).reshape(tok, hidden)
        total = jnp.zeros((tok, width), jnp.float32)
        for part in range(N_MP):
            rows = mixed[:, part * block:(part + 1) * block]
            low_out = jnp.dot(rows, o_left[index, part * block:(part + 1) * block], preferred_element_type=jnp.float32)
            term = jnp.dot(rows, w_out[part * block:(part + 1) * block], preferred_element_type=jnp.float32)
            term = term + noise_scale * sign * jnp.dot(low_out, o_right[index].astype(jnp.float32), precision=lax.Precision.HIGHEST)
            rounded = lax.optimization_barrier(term.astype(jnp.bfloat16))
            total = total + rounded.astype(jnp.float32)
        diff = total - target_f
        return -(jnp.sum(diff * diff) / (tok * width))
    fitness = lax.map(score, jnp.arange(members))
    mean = jnp.sum(fitness) / members
    spread = jnp.sum((fitness - mean) * (fitness - mean)) / members
    weight = signs * (fitness - mean) / jnp.sqrt(spread + spread_floor)
    left_q = jnp.transpose(query_left_factors.astype(jnp.float32) * weight[:, None, None], (1, 0, 2)).reshape(width, members * RANK)
    right_q = query_right_factors.astype(jnp.float32).reshape(members * RANK, hidden)
    grad_query = jnp.dot(left_q, right_q, precision=lax.Precision.HIGHEST) / noise_scale
    output_left_factor = jnp.transpose(o_left.astype(jnp.float32) * weight[:, None, None], (1, 0, 2)).reshape(hidden, members * RANK)
    right_o = o_right.astype(jnp.float32).reshape(members * RANK, width)
    grad_out = jnp.dot(output_left_factor, right_o, precision=lax.Precision.HIGHEST) / noise_scale
    return (grad_query, grad_out, fitness)
```

```python
import functools
import math

import jax
import jax.numpy as jnp
from jax import lax
from jax.experimental import pallas as pl
from jax.experimental.pallas import tpu as pltpu
from jax.sharding import Mesh
from jax.sharding import PartitionSpec as P

D = 3584
HEADS = 28
KV_HEADS = 4
HEAD_DIM = 128
RANK = 4
NX, NZ, NC, NY = 4, 8, 2, 4
PLANE = NX * NZ * NC
ROWS = D // PLANE
COLS = D // NY
AXES = ("pop_0", "pop_1", "pop_2", "mp")
POP = AXES[:3]
MESH = pl.DeviceIdType.MESH

noise_scale = 0.5
rope_base = 1000000.0
spread_floor = 0.001


def place():
    return tuple(lax.axis_index(a) for a in AXES)


def plane_device(p, y):
    return (p // (NZ * NC), (p // NC) % NZ, p % NC, y)


def meet_plane(me):
    x, z, c, y = me
    p = (x * NZ + z) * NC + c
    barrier = pltpu.get_barrier_semaphore()

    @pl.loop(1, PLANE)
    def _(i):
        pl.semaphore_signal(
            barrier, inc=1, device_id=plane_device((p + i) % PLANE, y), device_id_type=MESH
        )

    return barrier, PLANE - 1


def local_wait(ref, sem):
    pltpu.make_async_copy(ref, ref, sem).wait()


class PlaneGather:
    SEMS = 49

    def __init__(self, me, buf, sem, cut):
        self.x, self.z, self.c, self.y = me
        self.buf, self.sem = buf, sem
        self.a = pl.ds(0, cut)
        self.b = pl.ds(cut, COLS - cut)

    def zat(self, d):
        return (self.z + d + NZ) % NZ

    def xat(self, d):
        return (self.x + d + NX) % NX

    def send(self, ref, to, ssem, rsem):
        pltpu.make_async_remote_copy(
            src_ref=ref,
            dst_ref=ref,
            send_sem=self.sem.at[ssem],
            recv_sem=self.sem.at[rsem],
            device_id=to,
            device_id_type=MESH,
        ).start()

    def xdev(self, d):
        return (self.xat(d), self.z, self.c, self.y)

    def zdev(self, d):
        return (self.x, self.zat(d), self.c, self.y)

    def share(self, ref):
        self.send(ref, (self.x, self.z, 1 - self.c, self.y), 4, 5)

    def ra(self, right, s, h):
        return (7 if right else 15) + (s - 1) * 2 + h

    def rb(self, right, s):
        return (23 if right else 27) + s - 1

    def rx(self, right, k):
        return (31 if right else 39) + k

    @staticmethod
    def zoff(k):
        return -((k + 1) // 2) if k % 2 else k // 2

    def start(self):
        own_a = self.buf.at[self.x, self.z, self.c, :, self.a]
        own_b = self.buf.at[self.x, self.z, self.c, :, self.b]
        for d in (1, 3, 2):
            self.send(own_a, self.xdev(d), 0, 6)
        self.send(own_b, self.zdev(1), 2, self.rb(True, 1))
        self.send(own_b, self.zdev(-1), 2, self.rb(False, 1))
        self.send(own_b, self.xdev(1), 3, self.rx(True, 0))
        self.send(own_b, self.xdev(-1), 3, self.rx(False, 0))
        self.share(own_b)

    def a_line(self):
        local_wait(self.buf.at[pl.ds(0, 3), self.z, self.c, :, self.a], self.sem.at[6])
        for h in range(2):
            ref = self.buf.at[pl.ds(2 * h, 2), self.z, self.c, :, self.a]
            self.send(ref, self.zdev(1), 1, self.ra(True, 1, h))
            self.send(ref, self.zdev(-1), 1, self.ra(False, 1, h))
        self.share(self.buf.at[:, self.z, self.c, :, self.a])

    @staticmethod
    def a_moves(right, s, h):
        return s < 4 or (s == 4 and h == (0 if right else 1))

    def a_step(self, s):
        for h in range(2):
            for right in (True, False):
                if not self.a_moves(right, s, h):
                    continue
                zz = self.zat(-s if right else s)
                ref = self.buf.at[pl.ds(2 * h, 2), zz, self.c, :, self.a]
                local_wait(ref, self.sem.at[self.ra(right, s, h)])
                if s < 4 and self.a_moves(right, s + 1, h):
                    self.send(ref, self.zdev(1 if right else -1), 1, self.ra(right, s + 1, h))
                self.share(ref)

    def b_step(self, s):
        for right in (True, False):
            if s == 4 and not right:
                continue
            zz = self.zat(-s if right else s)
            k = 2 * s - 1 if right else 2 * s
            ref = self.buf.at[self.x, zz, self.c, :, self.b]
            local_wait(ref, self.sem.at[self.rb(right, s)])
            if s < 3 or (s == 3 and right):
                self.send(ref, self.zdev(1 if right else -1), 2, self.rb(right, s + 1))
            self.send(ref, self.xdev(1), 3, self.rx(True, k))
            self.send(ref, self.xdev(-1), 3, self.rx(False, k))
            self.share(ref)

    def x_step(self, k):
        zz = self.zat(self.zoff(k))
        for right in (True, False):
            ref = self.buf.at[self.xat(-1 if right else 1), zz, self.c, :, self.b]
            local_wait(ref, self.sem.at[self.rx(right, k)])
            if (k % 2 == 0) == right:
                self.send(ref, self.xdev(1 if right else -1), 3, 47 if right else 48)
            self.share(ref)

    def far(self):
        for s in (47, 48):
            local_wait(self.buf.at[0, pl.ds(0, 4), self.c, :, self.b], self.sem.at[s])
        self.share(self.buf.at[self.xat(2), :, self.c, :, self.b])

    def finish(self):
        local_wait(self.buf.at[:, :, 1 - self.c], self.sem.at[5])

    def drain(self):
        local_wait(self.buf.at[pl.ds(0, 3), 0, 0, :, self.a], self.sem.at[0])
        local_wait(self.buf.at[:, pl.ds(0, 7), 0, :, self.a], self.sem.at[1])
        local_wait(self.buf.at[0, pl.ds(0, 7), 0, :, self.b], self.sem.at[2])
        local_wait(self.buf.at[pl.ds(0, 3), :, 0, :, self.b], self.sem.at[3])
        local_wait(self.buf.at[:, :, self.c], self.sem.at[4])

    def run(self):
        self.a_line()
        for s in range(1, 5):
            self.b_step(s)
            for k in ((0,), (1, 2), (3, 4), (5, 6))[s - 1]:
                self.x_step(k)
            self.a_step(s)
        self.x_step(7)
        self.far()
        self.finish()


CUT = 384


def gather_kernel(wq, fac, wo, s_in, g1, g2, s_out, sem1, sem2, sem_s, sem_l):
    me = place()
    x, z, c, y = me
    p = (x * NZ + z) * NC + c
    barrier, expected = meet_plane(me)
    own = [
        pltpu.make_async_copy(wq, g1.at[x, z, c, pl.ds(0, ROWS), :], sem_l.at[0]),
        pltpu.make_async_copy(fac, g1.at[x, z, c, pl.ds(ROWS, 8), :], sem_l.at[1]),
        pltpu.make_async_copy(wo, g2.at[x, z, c], sem_l.at[2]),
    ]
    for copy in own:
        copy.start()
    s_out[p] = s_in[p]
    for copy in own:
        copy.wait()
    pl.semaphore_wait(barrier, expected)
    first = PlaneGather(me, g1, sem1, CUT)
    second = PlaneGather(me, g2, sem2, CUT)
    first.start()

    @pl.loop(1, PLANE)
    def _(i):
        to = (p + i) % PLANE
        pltpu.make_async_remote_copy(
            src_ref=s_in.at[to],
            dst_ref=s_out.at[p],
            send_sem=sem_s.at[0],
            recv_sem=sem_s.at[1],
            device_id=plane_device(to, y),
            device_id_type=MESH,
        ).start()

    second.start()
    first.run()
    second.run()
    local_wait(s_out.at[pl.ds(0, PLANE - 1)], sem_s.at[1])
    local_wait(s_out.at[pl.ds(0, PLANE - 1)], sem_s.at[0])
    first.drain()
    second.drain()


def gather_all(wq, fac, wo, s_in):
    return pl.pallas_call(
        gather_kernel,
        name="gather_all",
        out_shape=(
            jax.ShapeDtypeStruct((NX, NZ, NC, ROWS + 8, COLS), jnp.bfloat16),
            jax.ShapeDtypeStruct((NX, NZ, NC, ROWS, COLS), jnp.bfloat16),
            jax.ShapeDtypeStruct(s_in.shape, s_in.dtype),
        ),
        in_specs=[pl.BlockSpec(memory_space=pl.ANY)] * 3 + [pl.BlockSpec(memory_space=pltpu.VMEM)],
        out_specs=[pl.BlockSpec(memory_space=pltpu.VMEM)] * 3,
        scratch_shapes=[
            pltpu.SemaphoreType.DMA((PlaneGather.SEMS,)),
            pltpu.SemaphoreType.DMA((PlaneGather.SEMS,)),
            pltpu.SemaphoreType.DMA((2,)),
            pltpu.SemaphoreType.DMA((3,)),
        ],
        compiler_params=pltpu.CompilerParams(
            collective_id=0, has_side_effects=True, vmem_limit_bytes=56 * 1024 * 1024
        ),
    )(wq, fac, wo, s_in)


def exchange_kernel(t_ref, r_ref, fwd, ssem, rsem):
    x, z, c, y = place()
    up, down, far = (y + 1) % NY, (y + NY - 1) % NY, (y + 2) % NY
    half = COLS // 2
    lo, hi = pl.ds(0, half), pl.ds(half, half)
    barrier = pltpu.get_barrier_semaphore()
    for to in (up, down):
        pl.semaphore_signal(barrier, inc=1, device_id=(x, z, c, to), device_id_type=MESH)
    pl.semaphore_wait(barrier, 2)

    def send(src, dst, to, k):
        copy = pltpu.make_async_remote_copy(
            src_ref=src,
            dst_ref=dst,
            send_sem=ssem.at[k],
            recv_sem=rsem.at[k],
            device_id=(x, z, c, to),
            device_id_type=MESH,
        )
        copy.start()
        return copy

    copies = [
        send(t_ref.at[far, lo], fwd.at[0], up, 0),
        send(t_ref.at[far, hi], fwd.at[1], down, 1),
        send(t_ref.at[up], r_ref.at[y], up, 2),
        send(t_ref.at[down], r_ref.at[y], down, 3),
    ]
    r_ref[y] = t_ref[y]
    copies[0].wait_recv()
    copies.append(send(fwd.at[0], r_ref.at[down, lo], up, 4))
    copies[1].wait_recv()
    copies.append(send(fwd.at[1], r_ref.at[up, hi], down, 5))
    for copy in copies[2:]:
        copy.wait_recv()
    for copy in copies:
        copy.wait_send()


def exchange(terms):
    tok = terms.shape[2]
    return pl.pallas_call(
        exchange_kernel,
        name="exchange",
        out_shape=jax.ShapeDtypeStruct(terms.shape, terms.dtype),
        in_specs=[pl.BlockSpec(memory_space=pltpu.VMEM)],
        out_specs=pl.BlockSpec(memory_space=pltpu.VMEM),
        scratch_shapes=[
            pltpu.VMEM((2, COLS // 2, tok), terms.dtype),
            pltpu.SemaphoreType.DMA((6,)),
            pltpu.SemaphoreType.DMA((6,)),
        ],
        compiler_params=pltpu.CompilerParams(collective_id=1, has_side_effects=True),
    )(terms)


def scores_kernel(e_ref, out_ref, part, total, sem):
    me = place()
    x, z, c, y = me
    p = (x * NZ + z) * NC + c
    barrier, expected = meet_plane(me)
    for d in range(1, NY):
        pl.semaphore_signal(barrier, inc=1, device_id=(x, z, c, (y + d) % NY), device_id_type=MESH)
    part[y] = e_ref[...]
    pl.semaphore_wait(barrier, expected + NY - 1)
    for d in range(1, NY):
        pltpu.make_async_remote_copy(
            src_ref=e_ref,
            dst_ref=part.at[y],
            send_sem=sem.at[0],
            recv_sem=sem.at[1],
            device_id=(x, z, c, (y + d) % NY),
            device_id_type=MESH,
        ).start()
    local_wait(part.at[pl.ds(0, NY - 1)], sem.at[1])
    total[...] = part[0] + part[1] + part[2] + part[3]
    out_ref[p] = total[...]

    @pl.loop(1, PLANE)
    def _(i):
        pltpu.make_async_remote_copy(
            src_ref=total,
            dst_ref=out_ref.at[p],
            send_sem=sem.at[2],
            recv_sem=sem.at[3],
            device_id=plane_device((p + i) % PLANE, y),
            device_id_type=MESH,
        ).start()

    local_wait(out_ref.at[pl.ds(0, PLANE - 1)], sem.at[3])
    local_wait(part.at[pl.ds(0, NY - 1)], sem.at[0])
    local_wait(out_ref.at[pl.ds(0, PLANE - 1)], sem.at[2])


def everyone_scores(errors):
    return pl.pallas_call(
        scores_kernel,
        name="everyone_scores",
        out_shape=jax.ShapeDtypeStruct((PLANE, 1, 128), jnp.float32),
        in_specs=[pl.BlockSpec(memory_space=pltpu.VMEM)],
        out_specs=pl.BlockSpec(memory_space=pltpu.VMEM),
        scratch_shapes=[
            pltpu.VMEM((NY, 1, 128), jnp.float32),
            pltpu.VMEM((1, 128), jnp.float32),
            pltpu.SemaphoreType.DMA((4,)),
        ],
        compiler_params=pltpu.CompilerParams(collective_id=2, has_side_effects=True),
    )(errors)


def tables(count, head_size):
    position = jnp.arange(count, dtype=jnp.float32)
    index = jnp.arange(head_size // 2, dtype=jnp.float32)
    freq = jnp.exp(-math.log(rope_base) * 2.0 * index / head_size)
    angle = position[:, None] * freq[None, :]
    return (jnp.cos(angle)[:, None, :], jnp.sin(angle)[:, None, :])


def rotate(field, cosine_table, sine):
    half = field.shape[-1] // 2
    first = field[..., :half]
    second = field[..., half:]
    return jnp.concatenate(
        [first * cosine_table - second * sine, second * cosine_table + first * sine], axis=-1
    )


def per_device(
    tokens,
    target,
    w_query,
    w_key,
    w_value,
    w_out,
    query_left_factors,
    query_right_factors,
    o_left,
    o_right,
    member_ids,
):
    tok = tokens.shape[0]
    group = HEADS // KV_HEADS
    scale = HEAD_DIM ** (-0.5)
    f32 = jnp.float32
    cosine_table, sine = tables(tok, HEAD_DIM)

    signs = (1 - 2 * (member_ids % 2)).astype(f32)
    q_left_t = jnp.transpose(query_left_factors[0])
    o_left_t = jnp.transpose(o_left[0])
    fac = jnp.concatenate([query_right_factors[0], o_left_t], axis=0)
    both = jnp.concatenate([q_left_t, o_right[0]], axis=0)
    s_in = jnp.transpose(both.reshape(2 * RANK, PLANE, ROWS), (1, 0, 2))
    s_in = jnp.pad(s_in, ((0, 0), (0, 0), (0, 128 - ROWS))) * signs.astype(jnp.bfloat16)
    g1, g2, s_out = gather_all(w_query, fac, jnp.transpose(w_out), s_in)
    g1 = g1.reshape(PLANE, ROWS + 8, COLS)
    wide = jnp.pad(tokens.reshape(tok, PLANE, ROWS), ((0, 0), (0, 0), (0, 8)))
    base = jnp.dot(
        wide.reshape(tok, -1), g1.reshape(-1, COLS), preferred_element_type=f32
    )
    keys = rotate(
        jnp.dot(tokens, w_key, preferred_element_type=f32).reshape(tok, 1, HEAD_DIM),
        cosine_table,
        sine,
    ).astype(jnp.bfloat16)[:, 0]
    values = jnp.dot(tokens, w_value, preferred_element_type=f32).astype(jnp.bfloat16)
    factor = noise_scale * signs[0]
    low_q = jnp.dot(tokens, query_left_factors[0], preferred_element_type=f32).astype(jnp.bfloat16)
    query = base + factor * jnp.dot(low_q, query_right_factors[0], preferred_element_type=f32)
    query = rotate(query.reshape(tok, group, HEAD_DIM), cosine_table, sine).astype(jnp.bfloat16)
    scores = jnp.einsum("tgd,sd->gts", query, keys, preferred_element_type=f32) * scale
    causal = jnp.arange(tok)[:, None] >= jnp.arange(tok)[None, :]
    scores = jnp.where(causal, scores, -1e30)
    probs = jax.nn.softmax(scores, axis=-1).astype(jnp.bfloat16)
    mixed = (
        jnp.einsum("gts,sd->gdt", probs, values, preferred_element_type=f32)
        .astype(jnp.bfloat16)
        .reshape(COLS, tok)
    )
    low_o = jnp.dot(o_left_t, mixed, preferred_element_type=f32)
    part = jnp.dot(g2.reshape(D, COLS), mixed, preferred_element_type=f32)
    term = part + factor * jnp.einsum(
        "re,rt->et", o_right[0].astype(f32), low_o, precision=lax.Precision.HIGHEST
    )
    arrived = exchange(term.astype(jnp.bfloat16).reshape(NY, COLS, tok))
    output = jnp.sum(arrived.astype(f32), axis=0)
    diff = output - jnp.transpose(target).astype(f32)
    errors = jnp.full((1, 128), jnp.sum(diff * diff), f32)
    everyone = -(everyone_scores(errors)[:, 0, 0] / (tok * D))
    p = (lax.axis_index(POP[0]) * NZ + lax.axis_index(POP[1])) * NC + lax.axis_index(POP[2])
    fitness = lax.dynamic_slice(everyone, (p,), (1,))
    mean = jnp.sum(everyone) / PLANE
    spread = jnp.sum((everyone - mean) * (everyone - mean)) / PLANE
    unsigned = (everyone - mean) / jnp.sqrt(spread + spread_floor)
    lefts = s_out[:, :, :ROWS].astype(f32) * unsigned[:, None, None]
    rights = g1[:, ROWS:].astype(f32)

    def gradient(left, right):
        return (
            lax.dot_general(
                left.reshape(-1, ROWS),
                right.reshape(-1, COLS),
                (((0,), (0,)), ((), ())),
                precision=lax.Precision.HIGHEST,
            )
            / noise_scale
        )

    grad_query = gradient(lefts[:, :RANK], rights[:, :RANK])
    grad_out = gradient(lefts[:, RANK:], rights[:, RANK:])
    return (grad_query, jnp.transpose(grad_out), fitness)


def solution(mesh):
    torus = Mesh(mesh.devices.reshape(NX, NZ, NC, NY), AXES)
    placed = (
        P(),
        P(None, "mp"),
        P(POP, "mp"),
        P(None, "mp"),
        P(None, "mp"),
        P("mp", POP),
        P(POP, None, None),
        P(POP, None, "mp"),
        P(POP, "mp", None),
        P(POP, None, None),
        P(POP),
    )
    return jax.shard_map(
        per_device,
        mesh=torus,
        in_specs=placed,
        out_specs=(P(POP, "mp"), P("mp", POP), P(POP)),
        check_vma=False,
    )
```

```python
import math

import jax
import jax.numpy as jnp
import numpy as np
from jax import lax
from jax.experimental import pallas as pl
from jax.experimental.pallas import tpu as pltpu
from jax.sharding import Mesh
from jax.sharding import PartitionSpec as P

D = 3584
HEADS = 28
KV_HEADS = 4
HEAD_DIM = 128
RANK = 4
NX, NZ, NC, NY = 4, 8, 2, 4
PLANE = NX * NZ * NC
ROWS = D // PLANE
COLS = D // NY
AXES = ("pop_0", "pop_1", "pop_2", "mp")
POP = AXES[:3]
MESH = pl.DeviceIdType.MESH

noise_scale = 0.5
rope_base = 1000000.0
spread_floor = 0.001


def place():
    return tuple(lax.axis_index(a) for a in AXES)


def plane_device(p, y):
    return (p // (NZ * NC), (p // NC) % NZ, p % NC, y)


def meet_plane(me):
    x, z, c, y = me
    p = (x * NZ + z) * NC + c
    barrier = pltpu.get_barrier_semaphore()

    @pl.loop(1, PLANE)
    def _(i):
        pl.semaphore_signal(
            barrier, inc=1, device_id=plane_device((p + i) % PLANE, y), device_id_type=MESH
        )

    return barrier, PLANE - 1


def local_wait(ref, sem):
    pltpu.make_async_copy(ref, ref, sem).wait()


class PlaneGather:
    SEMS = 49

    def __init__(self, me, buf, sem, cut):
        self.x, self.z, self.c, self.y = me
        self.buf, self.sem = buf, sem
        self.a = pl.ds(0, cut)
        self.b = pl.ds(cut, COLS - cut)

    def zat(self, d):
        return (self.z + d + NZ) % NZ

    def yat(self, d):
        return (self.y + d + NY) % NY

    def send(self, ref, to, ssem, rsem):
        pltpu.make_async_remote_copy(
            src_ref=ref,
            dst_ref=ref,
            send_sem=self.sem.at[ssem],
            recv_sem=self.sem.at[rsem],
            device_id=to,
            device_id_type=MESH,
        ).start()

    def ydev(self, d):
        return (self.x, self.z, self.c, self.yat(d))

    def zdev(self, d):
        return (self.x, self.zat(d), self.c, self.y)

    def share(self, ref):
        self.send(ref, (self.x, self.z, 1 - self.c, self.y), 4, 5)

    def ra(self, right, s, h):
        return (7 if right else 15) + (s - 1) * 2 + h

    def rb(self, right, s):
        return (23 if right else 27) + s - 1

    def ry(self, right, k):
        return (31 if right else 39) + k

    @staticmethod
    def zoff(k):
        return -((k + 1) // 2) if k % 2 else k // 2

    def start(self):
        own_a = self.buf.at[self.y, self.z, self.c, :, self.a]
        own_b = self.buf.at[self.y, self.z, self.c, :, self.b]
        for d in (1, 3, 2):
            self.send(own_a, self.ydev(d), 0, 6)
        self.send(own_b, self.zdev(1), 2, self.rb(True, 1))
        self.send(own_b, self.zdev(-1), 2, self.rb(False, 1))
        self.send(own_b, self.ydev(1), 3, self.ry(True, 0))
        self.send(own_b, self.ydev(-1), 3, self.ry(False, 0))
        self.share(own_b)

    def a_line(self):
        local_wait(self.buf.at[pl.ds(0, 3), self.z, self.c, :, self.a], self.sem.at[6])
        for h in range(2):
            ref = self.buf.at[pl.ds(2 * h, 2), self.z, self.c, :, self.a]
            self.send(ref, self.zdev(1), 1, self.ra(True, 1, h))
            self.send(ref, self.zdev(-1), 1, self.ra(False, 1, h))
        self.share(self.buf.at[:, self.z, self.c, :, self.a])

    @staticmethod
    def a_moves(right, s, h):
        return s < 4 or (s == 4 and h == (0 if right else 1))

    def a_step(self, s):
        for h in range(2):
            for right in (True, False):
                if not self.a_moves(right, s, h):
                    continue
                zz = self.zat(-s if right else s)
                ref = self.buf.at[pl.ds(2 * h, 2), zz, self.c, :, self.a]
                local_wait(ref, self.sem.at[self.ra(right, s, h)])
                if s < 4 and self.a_moves(right, s + 1, h):
                    self.send(ref, self.zdev(1 if right else -1), 1, self.ra(right, s + 1, h))
                self.share(ref)

    def b_step(self, s):
        for right in (True, False):
            if s == 4 and not right:
                continue
            zz = self.zat(-s if right else s)
            k = 2 * s - 1 if right else 2 * s
            ref = self.buf.at[self.y, zz, self.c, :, self.b]
            local_wait(ref, self.sem.at[self.rb(right, s)])
            if s < 3 or (s == 3 and right):
                self.send(ref, self.zdev(1 if right else -1), 2, self.rb(right, s + 1))
            self.send(ref, self.ydev(1), 3, self.ry(True, k))
            self.send(ref, self.ydev(-1), 3, self.ry(False, k))
            self.share(ref)

    def y_step(self, k):
        zz = self.zat(self.zoff(k))
        for right in (True, False):
            ref = self.buf.at[self.yat(-1 if right else 1), zz, self.c, :, self.b]
            local_wait(ref, self.sem.at[self.ry(right, k)])
            if (k % 2 == 0) == right:
                self.send(ref, self.ydev(1 if right else -1), 3, 47 if right else 48)
            self.share(ref)

    def far(self):
        for s in (47, 48):
            local_wait(self.buf.at[0, pl.ds(0, 4), self.c, :, self.b], self.sem.at[s])
        self.share(self.buf.at[self.yat(2), :, self.c, :, self.b])

    def finish(self):
        local_wait(self.buf.at[:, :, 1 - self.c], self.sem.at[5])

    def drain(self):
        local_wait(self.buf.at[pl.ds(0, 3), 0, 0, :, self.a], self.sem.at[0])
        local_wait(self.buf.at[:, pl.ds(0, 7), 0, :, self.a], self.sem.at[1])
        local_wait(self.buf.at[0, pl.ds(0, 7), 0, :, self.b], self.sem.at[2])
        local_wait(self.buf.at[pl.ds(0, 3), :, 0, :, self.b], self.sem.at[3])
        local_wait(self.buf.at[:, :, self.c], self.sem.at[4])


CUT = 256
SLAB = 16
FAR_FIRST = (1, 7, 2, 6, 3, 5, 4)


def remote(src, dst, ssem, rsem, to):
    pltpu.make_async_remote_copy(
        src_ref=src, dst_ref=dst, send_sem=ssem, recv_sem=rsem, device_id=to, device_id_type=MESH
    ).start()


def forward_kernel(
    tok_h, wk_h, wv_h, wo_h, tgt_h, s_h, fac_h, lft_h, cos_h, sin_h,
    ev, fac_all, s_out,
    tok, wk, wv, tgt, s_in, fac, lft, cos, sin,
    wbuf, bt, mt, k4, v4, fb, lft_m, tgt_m, tgt_t, acc, low, part, total,
    sem_l, sem_w, sem_s, sem_t, sem_k, sem_1, sem_2, sem_3, sem_4, sem_f, sem_e,
):
    me = place()
    x, z, c, y = me
    p = (x * NZ + z) * NC + c
    f32, bf16 = jnp.float32, jnp.bfloat16
    tokens_n = tok.shape[0]
    half = HEAD_DIM // 2

    loads = {}
    for i, (name, src, dst) in enumerate(
        (
            ("wo", wo_h, wbuf.at[y, z, c]),
            ("s", s_h, s_in),
            ("lft", lft_h, lft),
            ("fac", fac_h, fac),
            ("own", fac_h, fac_all.at[x * NZ + z, c]),
            ("tgt", tgt_h, tgt),
            ("tok", tok_h, tok),
            ("wk", wk_h, wk),
            ("wv", wv_h, wv),
            ("cos", cos_h, cos),
            ("sin", sin_h, sin),
        )
    ):
        loads[name] = pltpu.make_async_copy(src, dst, sem_l.at[i])
        loads[name].start()

    barrier = pltpu.get_barrier_semaphore()

    def greet(to):
        pl.semaphore_signal(barrier, inc=1, device_id=to, device_id_type=MESH)

    @pl.loop(1, PLANE)
    def _(i):
        greet(plane_device((p + i) % PLANE, y))

    @pl.loop(0, 3 * NZ * NC)
    def _(i):
        greet((x, (i // NC) % NZ, i % NC, (y + 1 + i // (NZ * NC)) % NY))

    for dx in range(1, NX):
        for dy in range(1, NY):
            greet(((x + dx) % NX, z, c, (y + dy) % NY))

    fb[:, :, pl.ds(COLS, 128)] = jnp.zeros((NY, 8, 128), bf16)
    pl.semaphore_wait(barrier, PLANE - 1 + 3 * NZ * NC + 9)

    wide = PlaneGather(me, wbuf, sem_w, CUT)
    loads["s"].wait()

    @pl.loop(1, PLANE)
    def _(i):
        to = (p + i) % PLANE
        remote(s_in.at[to], s_out.at[p], sem_s.at[0], sem_s.at[1], plane_device(to, y))

    for name in ("lft", "fac", "tgt"):
        loads[name].wait()

    @pl.when(x != y)
    def _():
        remote(lft, lft_m, sem_t.at[0], sem_t.at[1], (y, z, c, x))
        remote(fac, fb.at[y, :, pl.ds(0, COLS)], sem_t.at[4], sem_t.at[5], (x, z, c, x))
        remote(tgt, tgt_m, sem_t.at[2], sem_t.at[3], (y, z, c, x))

    for d in range(1, NX):
        remote(fac, fb.at[y, :, pl.ds(0, COLS)], sem_t.at[4], sem_t.at[5], ((x + d) % NX, z, c, x))

    @pl.when(x == y)
    def _():
        lft_m[...] = lft[...]
        fb[y, :, pl.ds(0, COLS)] = fac[...]
        tgt_m[...] = tgt[...]

    loads["wo"].wait()
    wide.start()
    s_out[p] = s_in[p]

    for name in ("tok", "wk", "wv", "cos", "sin"):
        loads[name].wait()

    def turned(v):
        first, second = v[:half], v[half:]
        ct, st = cos[...], sin[...]
        return jnp.concatenate([first * ct - second * st, second * ct + first * st], axis=0)

    key_t = jnp.dot(tok[...], wk[...], preferred_element_type=f32).T
    k4[y] = turned(key_t).T.astype(bf16)
    v4[y] = jnp.dot(tok[...], wv[...], preferred_element_type=f32).T.astype(bf16)
    for d in range(1, NY):
        to = (x, z, c, (y + d) % NY)
        remote(k4.at[y], k4.at[y], sem_k.at[0], sem_k.at[1], to)
        remote(v4.at[y], v4.at[y], sem_k.at[2], sem_k.at[3], to)

    wide.a_line()

    @pl.when(x != y)
    def _():
        local_wait(lft_m, sem_t.at[1])

    local_wait(s_out.at[pl.ds(0, PLANE - 1)], sem_s.at[1])
    slab = jnp.concatenate([s_out[i, pl.ds(0, SLAB), pl.ds(0, ROWS)] for i in range(PLANE)], axis=1)
    made = lax.dot_general(
        jnp.concatenate([slab, lft_m[...]], axis=0),
        tok[...],
        (((1,), (1,)), ((), ())),
        preferred_element_type=f32,
    )
    bt[y, x, z, c] = made[:SLAB].astype(bf16)
    low[...] = made[SLAB : SLAB + 8].astype(bf16)
    for d in range(1, NY):
        own = bt.at[y, x, z, c]
        remote(own, own, sem_1.at[0], sem_1.at[1], (x, z, c, (y + d) % NY))

    wide.b_step(1)
    wide.y_step(0)

    @pl.when(x != y)
    def _():
        local_wait(tgt_m, sem_t.at[3])

    tgt_t[...] = tgt_m[...].astype(f32).T

    local_wait(bt.at[pl.ds(0, 3), 0, 0, 0], sem_1.at[1])

    def line_out(zz):
        ref = bt.at[:, x, zz, c]
        for d in (1, 3, 2):
            remote(ref, ref, sem_3.at[0], sem_3.at[d], ((x + d) % NX, z, c, y))
        remote(ref, ref, sem_4.at[0], sem_4.at[1], (x, z, 1 - c, y))

    mine = bt.at[:, x, z, c]
    for d in FAR_FIRST:
        remote(mine, mine, sem_2.at[0], sem_2.at[d], (x, (z + d) % NZ, c, y))
    line_out(z)

    def line_in(d):
        zz = (z + NZ - d) % NZ
        local_wait(bt.at[:, x, zz, c], sem_2.at[d])
        line_out(zz)

    wide.a_step(1)
    for d in FAR_FIRST[:3]:
        line_in(d)
    wide.b_step(2)
    wide.y_step(1)
    wide.y_step(2)
    for d in FAR_FIRST[3:]:
        line_in(d)
    wide.a_step(2)

    row = lax.broadcasted_iota(jnp.int32, (tokens_n, tokens_n), 0)
    col = lax.broadcasted_iota(jnp.int32, (tokens_n, tokens_n), 1)

    def attend(xb):
        @pl.loop(0, NY)
        def _(yh):
            right = fb[yh, pl.ds(0, RANK), pl.ds(pl.multiple_of(xb * 256, 256), 256)]
            shift = lax.dot_general(
                right, low[pl.ds(0, RANK), :], (((0,), (0,)), ((), ())), preferred_element_type=f32
            )
            base = bt[yh, xb].reshape(2 * HEAD_DIM, tokens_n).astype(f32)
            query = base + noise_scale * shift
            for j in range(2):
                q = turned(query[j * HEAD_DIM : (j + 1) * HEAD_DIM]).astype(bf16)
                scores = jnp.dot(k4[yh], q, preferred_element_type=f32) * HEAD_DIM ** (-0.5)
                scores = jnp.where(row <= col, scores, -1e30)
                scores = jnp.exp(scores - jnp.max(scores, axis=0, keepdims=True))
                probs = scores / jnp.sum(scores, axis=0, keepdims=True)
                mixed = jnp.dot(v4[yh], probs.astype(bf16), preferred_element_type=f32)
                mt[yh, xb * 2 + j] = mixed.astype(bf16)

    local_wait(bt.at[:, x, :, 1 - c], sem_4.at[1])
    for k in (1, 3):
        local_wait(k4.at[pl.ds(0, 3)] if k == 1 else v4.at[pl.ds(0, 3)], sem_k.at[k])

    @pl.when(x != y)
    def _():
        local_wait(fb.at[:, :, pl.ds(0, COLS)], sem_t.at[5])

    @pl.when(x == y)
    def _():
        local_wait(fb.at[pl.ds(0, 3), :, pl.ds(0, COLS)], sem_t.at[5])

    attend(x)
    wide.b_step(3)
    wide.y_step(3)
    wide.y_step(4)
    wide.a_step(3)

    def block_in(d):
        ref = bt.at[:, (x + NX - d) % NX, :, c]
        local_wait(ref, sem_3.at[d])
        remote(ref, ref, sem_4.at[0], sem_4.at[1 + d], (x, z, 1 - c, y))

    def block_use(d):
        xb = (x + NX - d) % NX
        local_wait(bt.at[:, xb, :, 1 - c], sem_4.at[1 + d])
        attend(xb)

    block_in(1)
    block_in(3)
    wide.b_step(4)
    wide.y_step(5)
    wide.y_step(6)
    wide.a_step(4)
    block_in(2)
    wide.y_step(7)
    wide.far()
    chip = x * NZ + z
    own = fac_all.at[chip, c]
    loads["own"].wait()

    @pl.loop(1, NX * NZ)
    def _(i):
        to = (chip + i) % (NX * NZ)
        remote(own, own, sem_f.at[0], sem_f.at[1], (to // NZ, to % NZ, c, y))

    block_use(1)
    block_use(3)
    block_use(2)

    wide.finish()
    out_right = lft_m[pl.ds(RANK, RANK), pl.ds(pl.multiple_of(x * COLS, 128), COLS)].astype(f32)
    acc[...] = -tgt_t[...]

    @pl.loop(0, NY)
    def _(b):
        rows = mt[b, pl.ds(0, 7)].reshape(COLS, tokens_n)
        term = jnp.dot(wbuf[b].reshape(COLS, COLS), rows, preferred_element_type=f32)
        low_o = jnp.dot(fb[b, pl.ds(RANK, RANK), pl.ds(0, COLS)], rows, preferred_element_type=f32)
        shift = lax.dot_general(
            out_right,
            low_o,
            (((0,), (0,)), ((), ())),
            precision=lax.Precision.HIGHEST,
            preferred_element_type=f32,
        )
        acc[...] += (term + noise_scale * shift).astype(bf16).astype(f32)

    part[x] = jnp.full((1, 128), jnp.sum(acc[...] * acc[...]), f32)
    for d in range(1, NX):
        remote(part.at[x], part.at[x], sem_e.at[0], sem_e.at[1], ((x + d) % NX, z, c, y))
    local_wait(fac_all.at[pl.ds(0, NX * NZ - 1), c], sem_f.at[1])
    remote(fac_all.at[:, c], fac_all.at[:, c], sem_f.at[2], sem_f.at[3], (x, z, 1 - c, y))
    local_wait(part.at[pl.ds(0, NX - 1)], sem_e.at[1])
    total[...] = part[0] + part[1] + part[2] + part[3]
    slot = (y * NZ + z) * NC + c
    ev[slot] = total[...]

    @pl.loop(1, PLANE)
    def _(i):
        to = (slot + i) % PLANE
        remote(
            total,
            ev.at[slot],
            sem_e.at[2],
            sem_e.at[3],
            (x, (to // NC) % NZ, to % NC, to // (NZ * NC)),
        )

    local_wait(ev.at[pl.ds(0, PLANE - 1)], sem_e.at[3])
    local_wait(fac_all.at[:, 1 - c], sem_f.at[3])

    wide.drain()
    local_wait(s_out.at[pl.ds(0, PLANE - 1)], sem_s.at[0])

    @pl.when(x != y)
    def _():
        local_wait(lft_m, sem_t.at[0])
        local_wait(tgt_m, sem_t.at[2])
        local_wait(fb.at[:, :, pl.ds(0, COLS)], sem_t.at[4])

    @pl.when(x == y)
    def _():
        local_wait(fb.at[pl.ds(0, 3), :, pl.ds(0, COLS)], sem_t.at[4])

    local_wait(k4.at[pl.ds(0, 3)], sem_k.at[0])
    local_wait(v4.at[pl.ds(0, 3)], sem_k.at[2])
    local_wait(bt.at[pl.ds(0, 3), 0, 0, 0], sem_1.at[0])
    local_wait(bt.at[:, 0, pl.ds(0, 7), 0], sem_2.at[0])
    local_wait(bt.at[:, pl.ds(0, 3), :, 0], sem_3.at[0])
    local_wait(bt.at[:, :, :, 0], sem_4.at[0])
    local_wait(fac_all.at[pl.ds(0, NX * NZ - 1), c], sem_f.at[0])
    local_wait(fac_all.at[:, c], sem_f.at[2])
    local_wait(part.at[pl.ds(0, NX - 1)], sem_e.at[0])
    local_wait(ev.at[pl.ds(0, PLANE - 1)], sem_e.at[2])


def forward(tokens, w_key, w_value, wo_t, target, s_in, fac, lft, cos_t, sin_t):
    tok = tokens.shape[0]
    bf16, f32 = jnp.bfloat16, jnp.float32
    ins = (tokens, w_key, w_value, wo_t, target, s_in, fac, lft, cos_t, sin_t)
    held = (tokens, w_key, w_value, target, s_in, fac, lft, cos_t, sin_t)
    dma = pltpu.SemaphoreType.DMA
    return pl.pallas_call(
        forward_kernel,
        name="forward",
        out_shape=(
            jax.ShapeDtypeStruct((PLANE, 1, 128), f32),
            jax.ShapeDtypeStruct((NX * NZ, NC, 8, COLS), bf16),
            jax.ShapeDtypeStruct(s_in.shape, bf16),
        ),
        in_specs=[pl.BlockSpec(memory_space=pl.ANY)] * len(ins),
        out_specs=[pl.BlockSpec(memory_space=pltpu.VMEM)] * 3,
        scratch_shapes=[pltpu.VMEM(a.shape, a.dtype) for a in held]
        + [
            pltpu.VMEM((NY, NZ, NC, ROWS, COLS), bf16),
            pltpu.VMEM((NY, NX, NZ, NC, SLAB, tok), bf16),
            pltpu.VMEM((NY, 8, HEAD_DIM, tok), bf16),
            pltpu.VMEM((NY, tok, HEAD_DIM), bf16),
            pltpu.VMEM((NY, HEAD_DIM, tok), bf16),
            pltpu.VMEM((NY, 8, COLS + 128), bf16),
            pltpu.VMEM((8, D), bf16),
            pltpu.VMEM((tok, COLS), bf16),
            pltpu.VMEM((COLS, tok), f32),
            pltpu.VMEM((COLS, tok), f32),
            pltpu.VMEM((8, tok), bf16),
            pltpu.VMEM((NX, 1, 128), f32),
            pltpu.VMEM((1, 128), f32),
            dma((11,)),
            dma((PlaneGather.SEMS,)),
            dma((2,)),
            dma((6,)),
            dma((4,)),
            dma((2,)),
            dma((8,)),
            dma((4,)),
            dma((5,)),
            dma((4,)),
            dma((4,)),
        ],
        compiler_params=pltpu.CompilerParams(
            collective_id=0, has_side_effects=True, vmem_limit_bytes=60 * 1024 * 1024
        ),
    )(*ins)


def tables(count, head_size):
    position = np.arange(count, dtype=np.float64)
    index = np.arange(head_size // 2, dtype=np.float64)
    freq = np.exp(-math.log(rope_base) * 2.0 * index / head_size)
    angle = freq[:, None] * position[None, :]
    return np.cos(angle).astype(np.float32), np.sin(angle).astype(np.float32)


def per_device(
    tokens,
    target,
    w_query,
    w_key,
    w_value,
    w_out,
    query_left_factors,
    query_right_factors,
    o_left,
    o_right,
    member_ids,
):
    tok = tokens.shape[0]
    f32, bf16 = jnp.float32, jnp.bfloat16
    cos_t, sin_t = tables(tok, HEAD_DIM)
    signs = (1 - 2 * (member_ids % 2)).astype(bf16)
    lft = jnp.concatenate([jnp.transpose(query_left_factors[0]), o_right[0]], axis=0) * signs
    fac = jnp.concatenate([query_right_factors[0], jnp.transpose(o_left[0])], axis=0)
    slabs = jnp.transpose(w_query).reshape(COLS // SLAB, SLAB, ROWS)
    slabs = jnp.pad(slabs, ((0, PLANE - COLS // SLAB), (0, 0), (0, 128 - ROWS)))
    lefts = jnp.transpose(lft.reshape(2 * RANK, PLANE, ROWS), (1, 0, 2))
    lefts = jnp.pad(lefts, ((0, 0), (0, 0), (0, 128 - ROWS)))
    s_in = jnp.concatenate([slabs, lefts], axis=1)
    errors, facs, s_out = forward(
        tokens, w_key, w_value, jnp.transpose(w_out), target, s_in, fac, lft, cos_t, sin_t
    )
    everyone = -(errors[:, 0, 0] / (tok * D))
    p = (lax.axis_index(POP[0]) * NZ + lax.axis_index(POP[1])) * NC + lax.axis_index(POP[2])
    fitness = lax.dynamic_slice(everyone, (p,), (1,))
    mean = jnp.sum(everyone) / PLANE
    spread = jnp.sum((everyone - mean) * (everyone - mean)) / PLANE
    unsigned = (everyone - mean) / jnp.sqrt(spread + spread_floor)
    lefts = s_out[:, SLAB:, :ROWS].astype(f32) * unsigned[:, None, None]
    rights = facs.reshape(PLANE, 2 * RANK, COLS).astype(f32)

    def gradient(left, right):
        return (
            lax.dot_general(
                left.reshape(-1, ROWS),
                right.reshape(-1, COLS),
                (((0,), (0,)), ((), ())),
                precision=lax.Precision.HIGHEST,
            )
            / noise_scale
        )

    grad_query = gradient(lefts[:, :RANK], rights[:, :RANK])
    grad_out = gradient(lefts[:, RANK:], rights[:, RANK:])
    return (grad_query, jnp.transpose(grad_out), fitness)


def solution(mesh):
    torus = Mesh(mesh.devices.reshape(NX, NZ, NC, NY), AXES)
    placed = (
        P(),
        P(None, "mp"),
        P(POP, "mp"),
        P(None, "mp"),
        P(None, "mp"),
        P("mp", POP),
        P(POP, None, None),
        P(POP, None, "mp"),
        P(POP, "mp", None),
        P(POP, None, None),
        P(POP),
    )
    return jax.shard_map(
        per_device,
        mesh=torus,
        in_specs=placed,
        out_specs=(P(POP, "mp"), P("mp", POP), P(POP)),
        check_vma=False,
    )
```

```python
import math

import jax
import jax.numpy as jnp
import numpy as np
from jax import lax
from jax.experimental import pallas as pl
from jax.experimental.pallas import tpu as pltpu
from jax.sharding import Mesh
from jax.sharding import PartitionSpec as P

D = 3584
HEADS = 28
KV_HEADS = 4
HEAD_DIM = 128
RANK = 4
NX, NZ, NC, NY = 4, 8, 2, 4
PLANE = NX * NZ * NC
ROWS = D // PLANE
COLS = D // NY
AXES = ("pop_0", "pop_1", "pop_2", "mp")
POP = AXES[:3]
MESH = pl.DeviceIdType.MESH

noise_scale = 0.5
rope_base = 1000000.0
spread_floor = 0.001


def place():
    return tuple(lax.axis_index(a) for a in AXES)


def plane_device(p, y):
    return (p // (NZ * NC), (p // NC) % NZ, p % NC, y)


def local_wait(ref, sem):
    pltpu.make_async_copy(ref, ref, sem).wait()


class PlaneGather:
    SEMS = 49

    def __init__(self, me, buf, sem, cut):
        self.x, self.z, self.c, self.y = me
        self.sem = sem
        self.buf = buf
        self.a = pl.ds(0, cut)
        self.b = pl.ds(cut, COLS - cut)

    def zat(self, d):
        return (self.z + d + NZ) % NZ

    def yat(self, d):
        return (self.y + d + NY) % NY

    def send(self, ref, to, ssem, rsem):
        pltpu.make_async_remote_copy(
            src_ref=ref,
            dst_ref=ref,
            send_sem=self.sem.at[ssem],
            recv_sem=self.sem.at[rsem],
            device_id=to,
            device_id_type=MESH,
        ).start()

    def ydev(self, d):
        return (self.x, self.z, self.c, self.yat(d))

    def zdev(self, d):
        return (self.x, self.zat(d), self.c, self.y)

    def share(self, ref):
        self.send(ref, (self.x, self.z, 1 - self.c, self.y), 4, 5)

    def ra(self, right, s, h):
        return (7 if right else 15) + (s - 1) * 2 + h

    def rb(self, right, s):
        return (23 if right else 27) + s - 1

    def ry(self, right, k):
        return (31 if right else 39) + k

    @staticmethod
    def zoff(k):
        return -((k + 1) // 2) if k % 2 else k // 2

    def start(self):
        own_a = self.buf.at[self.y, self.z, self.c, :, self.a]
        own_b = self.buf.at[self.y, self.z, self.c, :, self.b]
        for d in (1, 3, 2):
            self.send(own_a, self.ydev(d), 0, 6)
        self.send(own_b, self.zdev(1), 2, self.rb(True, 1))
        self.send(own_b, self.zdev(-1), 2, self.rb(False, 1))
        self.send(own_b, self.ydev(1), 3, self.ry(True, 0))
        self.send(own_b, self.ydev(-1), 3, self.ry(False, 0))
        self.share(own_b)

    def a_line(self):
        local_wait(self.buf.at[pl.ds(0, 3), self.z, self.c, :, self.a], self.sem.at[6])
        for h in range(2):
            ref = self.buf.at[pl.ds(2 * h, 2), self.z, self.c, :, self.a]
            self.send(ref, self.zdev(1), 1, self.ra(True, 1, h))
            self.send(ref, self.zdev(-1), 1, self.ra(False, 1, h))
        self.share(self.buf.at[:, self.z, self.c, :, self.a])

    @staticmethod
    def a_moves(right, s, h):
        return s < 4 or (s == 4 and h == (0 if right else 1))

    def a_step(self, s):
        for h in range(2):
            for right in (True, False):
                if not self.a_moves(right, s, h):
                    continue
                zz = self.zat(-s if right else s)
                ref = self.buf.at[pl.ds(2 * h, 2), zz, self.c, :, self.a]
                local_wait(ref, self.sem.at[self.ra(right, s, h)])
                if s < 4 and self.a_moves(right, s + 1, h):
                    self.send(ref, self.zdev(1 if right else -1), 1, self.ra(right, s + 1, h))
                self.share(ref)

    def b_step(self, s):
        for right in (True, False):
            if s == 4 and not right:
                continue
            zz = self.zat(-s if right else s)
            k = 2 * s - 1 if right else 2 * s
            ref = self.buf.at[self.y, zz, self.c, :, self.b]
            local_wait(ref, self.sem.at[self.rb(right, s)])
            if s < 3 or (s == 3 and right):
                self.send(ref, self.zdev(1 if right else -1), 2, self.rb(right, s + 1))
            self.send(ref, self.ydev(1), 3, self.ry(True, k))
            self.send(ref, self.ydev(-1), 3, self.ry(False, k))
            self.share(ref)

    def y_step(self, k):
        zz = self.zat(self.zoff(k))
        for right in (True, False):
            ref = self.buf.at[self.yat(-1 if right else 1), zz, self.c, :, self.b]
            local_wait(ref, self.sem.at[self.ry(right, k)])
            if (k % 2 == 0) == right:
                self.send(ref, self.ydev(1 if right else -1), 3, 47 if right else 48)
            self.share(ref)

    def far(self):
        for s in (47, 48):
            local_wait(self.buf.at[0, pl.ds(0, 4), self.c, :, self.b], self.sem.at[s])
        self.share(self.buf.at[self.yat(2), :, self.c, :, self.b])

    def finish(self):
        local_wait(self.buf.at[:, :, 1 - self.c, :, pl.ds(0, COLS)], self.sem.at[5])

    def drain(self):
        local_wait(self.buf.at[pl.ds(0, 3), 0, 0, :, self.a], self.sem.at[0])
        local_wait(self.buf.at[:, pl.ds(0, 7), 0, :, self.a], self.sem.at[1])
        local_wait(self.buf.at[0, pl.ds(0, 7), 0, :, self.b], self.sem.at[2])
        local_wait(self.buf.at[pl.ds(0, 3), :, 0, :, self.b], self.sem.at[3])
        local_wait(self.buf.at[:, :, self.c, :, pl.ds(0, COLS)], self.sem.at[4])


CUT = 256
SLAB = 16
FAR_FIRST = (1, 7, 2, 6, 3, 5, 4)


def remote(src, dst, ssem, rsem, to):
    pltpu.make_async_remote_copy(
        src_ref=src, dst_ref=dst, send_sem=ssem, recv_sem=rsem, device_id=to, device_id_type=MESH
    ).start()


def forward_kernel(
    ids, tok_h, wk_h, wv_h, wo_h, tgt_h, wq_h, ql_h, qr_h, ol_h, or_h, cos_h, sin_h,
    grad_q, grad_o, fit,
    tok, wk, wv, tgt, wq, ql, qr, ol, orr, cos, sin,
    slab_in, slab_out, left_in, left_out, fac, fac_all, lft, ev,
    wbuf, bt, mt, k4, v4, fb, lft_m, tgt_t, acc, low, part, total,
    sem_l, sem_w, sem_s, sem_t, sem_k, sem_1, sem_2, sem_3, sem_4, sem_f, sem_e, sem_g,
):
    me = place()
    x, z, c, y = me
    p = (x * NZ + z) * NC + c
    f32, bf16 = jnp.float32, jnp.bfloat16
    tokens_n = tok.shape[0]
    half = HEAD_DIM // 2
    sibling = (x, z, 1 - c, y)

    loads = {}
    for i, (name, src, dst) in enumerate(
        (
            ("wq", wq_h, wq),
            ("ql", ql_h, ql),
            ("or", or_h, orr),
            ("qr", qr_h, qr),
            ("ol", ol_h, ol),
            ("wo", wo_h, wbuf.at[y, z, c, :, pl.ds(0, COLS)]),
            ("tok", tok_h, tok),
            ("wk", wk_h, wk),
            ("wv", wv_h, wv),
            ("cos", cos_h, cos),
            ("sin", sin_h, sin),
            ("tgt", tgt_h, tgt),
        )
    ):
        loads[name] = pltpu.make_async_copy(src, dst, sem_l.at[i])
        loads[name].start()

    barrier = pltpu.get_barrier_semaphore()

    def greet(to):
        pl.semaphore_signal(barrier, inc=1, device_id=to, device_id_type=MESH)

    @pl.loop(1, PLANE)
    def _(i):
        greet(plane_device((p + i) % PLANE, y))

    @pl.loop(0, 3 * NZ * NC)
    def _(i):
        greet((x, (i // NC) % NZ, i % NC, (y + 1 + i // (NZ * NC)) % NY))

    for dx in range(1, NX):
        for dy in range(1, NY):
            greet(((x + dx) % NX, z, c, (y + dy) % NY))

    def turned(v):
        first, second = v[:half], v[half:]
        ct, st = cos[...], sin[...]
        return jnp.concatenate([first * ct - second * st, second * ct + first * st], axis=0)

    sign = (1 - 2 * (ids[0] % 2)).astype(f32)
    for name in ("wq", "ql", "or", "qr", "ol"):
        loads[name].wait()
    slab_in[pl.ds(0, COLS // SLAB), :, pl.ds(0, ROWS)] = (
        wq[...].astype(f32).T.reshape(COLS // SLAB, SLAB, ROWS).astype(bf16)
    )
    slab_in[pl.ds(COLS // SLAB, PLANE - COLS // SLAB)] = jnp.zeros(
        (PLANE - COLS // SLAB, SLAB, 128), bf16
    )
    fac[...] = jnp.concatenate([qr[...].astype(f32), ol[...].astype(f32)], axis=0).astype(bf16)
    lft[...] = (jnp.concatenate([ql[...].astype(f32), orr[...].astype(f32)], axis=0) * sign).astype(bf16)
    for i in range(PLANE):
        left_in[i, :, pl.ds(0, ROWS)] = lft[:, pl.ds(i * ROWS, ROWS)]
    fb[:, :, pl.ds(COLS, 128)] = jnp.zeros((NY, 8, 128), bf16)
    slab_out[p] = slab_in[p]
    left_out[p] = left_in[p]
    fac_all[x * NZ + z, c] = fac[...]

    for name in ("tok", "wk", "wv", "cos", "sin"):
        loads[name].wait()
    key_t = jnp.dot(tok[...], wk[...], preferred_element_type=f32).T
    k4[y] = turned(key_t).T.astype(bf16)
    v4[y] = jnp.dot(tok[...], wv[...], preferred_element_type=f32).T.astype(bf16)
    loads["wo"].wait()
    loads["tgt"].wait()
    pl.semaphore_wait(barrier, PLANE - 1 + 3 * NZ * NC + 9)

    @pl.loop(1, PLANE)
    def _(i):
        to = (p + i) % PLANE
        remote(slab_in.at[to], slab_out.at[p], sem_s.at[0], sem_s.at[1], plane_device(to, y))

    @pl.when(x != y)
    def _():
        remote(lft, lft_m, sem_t.at[0], sem_t.at[1], (y, z, c, x))

    wide = PlaneGather(me, wbuf, sem_w, CUT)
    wide.start()

    key_half = k4.at[y, pl.ds(pl.multiple_of(c * 128, 128), 128)]
    value_half = v4.at[y, pl.ds(pl.multiple_of(c * 64, 64), 64)]
    for d in range(1, NY):
        to = (x, z, c, (y + d) % NY)
        remote(key_half, key_half, sem_k.at[0], sem_k.at[1], to)
        remote(value_half, value_half, sem_k.at[2], sem_k.at[3], to)

    @pl.when(x == y)
    def _():
        lft_m[...] = lft[...]

    wide.a_line()

    @pl.when(x != y)
    def _():
        local_wait(lft_m, sem_t.at[1])

    local_wait(slab_out.at[pl.ds(0, PLANE - 1)], sem_s.at[1])
    slab = jnp.concatenate([slab_out[i, :, pl.ds(0, ROWS)] for i in range(PLANE)], axis=1)
    made = lax.dot_general(
        jnp.concatenate([slab, lft_m[...]], axis=0),
        tok[...],
        (((1,), (1,)), ((), ())),
        preferred_element_type=f32,
    )
    bt[y, x, z, c] = made[:SLAB].astype(bf16)
    low[...] = made[SLAB : SLAB + 8].astype(bf16)
    for d in range(1, NY):
        own = bt.at[y, x, z, c]
        remote(own, own, sem_1.at[0], sem_1.at[1], (x, z, c, (y + d) % NY))

    tgt_half = tgt.at[pl.ds(pl.multiple_of(c * 128, 128), 128)]

    @pl.when(x == y)
    def _():
        for d in range(1, NY):
            to = (x, z, c, (y + d) % NY)
            remote(tgt_half, tgt_half, sem_t.at[2], sem_t.at[3], to)

    spot = fb.at[y, :, pl.ds(0, COLS)]

    @pl.when(x != y)
    def _():
        remote(fac, spot, sem_t.at[4], sem_t.at[5], (x, z, c, x))

    for d in range(1, NX):
        remote(fac, spot, sem_t.at[4], sem_t.at[5], ((x + d) % NX, z, c, x))

    @pl.when(x == y)
    def _():
        fb[y, :, pl.ds(0, COLS)] = fac[...]

    wide.b_step(1)
    wide.y_step(0)

    local_wait(bt.at[pl.ds(0, 3), 0, 0, 0], sem_1.at[1])

    def line_out(zz):
        ref = bt.at[:, x, zz, c]
        for d in (1, 3, 2):
            remote(ref, ref, sem_3.at[0], sem_3.at[d], ((x + d) % NX, z, c, y))
        remote(ref, ref, sem_4.at[0], sem_4.at[1], (x, z, 1 - c, y))

    mine = bt.at[:, x, z, c]
    for d in FAR_FIRST:
        remote(mine, mine, sem_2.at[0], sem_2.at[d], (x, (z + d) % NZ, c, y))
    line_out(z)

    def line_in(d):
        zz = (z + NZ - d) % NZ
        local_wait(bt.at[:, x, zz, c], sem_2.at[d])
        line_out(zz)

    wide.a_step(1)
    for d in FAR_FIRST[:3]:
        line_in(d)
    wide.b_step(2)
    wide.y_step(1)
    wide.y_step(2)
    for d in FAR_FIRST[3:]:
        line_in(d)
    wide.a_step(2)

    local_wait(k4.at[pl.ds(0, 3), pl.ds(0, 128)], sem_k.at[1])
    keys_in = k4.at[:, pl.ds(pl.multiple_of(c * 128, 128), 128)]
    remote(keys_in, keys_in, sem_k.at[4], sem_k.at[5], sibling)
    local_wait(v4.at[pl.ds(0, 3), pl.ds(0, 64)], sem_k.at[3])
    values_in = v4.at[:, pl.ds(pl.multiple_of(c * 64, 64), 64)]
    remote(values_in, values_in, sem_k.at[7], sem_k.at[6], sibling)

    @pl.when(x != y)
    def _():
        local_wait(tgt_half, sem_t.at[3])
        remote(tgt_half, tgt_half, sem_t.at[6], sem_t.at[7], sibling)

    row = lax.broadcasted_iota(jnp.int32, (tokens_n, tokens_n), 0)
    col = lax.broadcasted_iota(jnp.int32, (tokens_n, tokens_n), 1)

    to_log2 = HEAD_DIM ** (-0.5) * math.log2(math.e)

    def attend(xb):
        @pl.loop(0, NY)
        def _(yh):
            right = fb[yh, pl.ds(0, RANK), pl.ds(pl.multiple_of(xb * 256, 256), 256)]
            shift = lax.dot_general(
                right, low[pl.ds(0, RANK), :], (((0,), (0,)), ((), ())), preferred_element_type=f32
            )
            base = bt[yh, xb].reshape(2 * HEAD_DIM, tokens_n).astype(f32)
            query = base + noise_scale * shift
            for j in range(2):
                q = turned(query[j * HEAD_DIM : (j + 1) * HEAD_DIM]).astype(bf16)
                scores = jnp.dot(k4[yh], q, preferred_element_type=f32)
                scores = jnp.where(row <= col, scores, -1e30)
                scores = jnp.exp2((scores - jnp.max(scores, axis=0, keepdims=True)) * to_log2)
                share = 1.0 / jnp.sum(scores, axis=0, keepdims=True)
                mixed = jnp.dot(v4[yh], (scores * share).astype(bf16), preferred_element_type=f32)
                mt[yh, xb * 2 + j] = mixed.astype(bf16)

    local_wait(bt.at[:, x, :, 1 - c], sem_4.at[1])
    local_wait(k4.at[:, pl.ds(0, 128)], sem_k.at[5])
    local_wait(v4.at[:, pl.ds(0, 64)], sem_k.at[6])

    @pl.when(x != y)
    def _():
        local_wait(fb.at[:, :, pl.ds(0, COLS)], sem_t.at[5])

    @pl.when(x == y)
    def _():
        local_wait(fb.at[pl.ds(0, 3), :, pl.ds(0, COLS)], sem_t.at[5])

    attend(x)
    wide.b_step(3)
    wide.y_step(3)
    wide.y_step(4)
    wide.a_step(3)

    def block_in(d):
        ref = bt.at[:, (x + NX - d) % NX, :, c]
        local_wait(ref, sem_3.at[d])
        remote(ref, ref, sem_4.at[0], sem_4.at[1 + d], (x, z, 1 - c, y))

    def block_use(d):
        xb = (x + NX - d) % NX
        local_wait(bt.at[:, xb, :, 1 - c], sem_4.at[1 + d])
        attend(xb)

    block_in(1)
    block_in(3)
    wide.b_step(4)
    wide.y_step(5)
    wide.y_step(6)
    wide.a_step(4)
    block_in(2)
    wide.y_step(7)
    wide.far()
    chip = x * NZ + z
    own = fac_all.at[chip, c]

    @pl.loop(1, NX * NZ)
    def _(i):
        to = (chip + i) % (NX * NZ)
        remote(fac, own, sem_f.at[0], sem_f.at[1], (to // NZ, to % NZ, c, y))

    @pl.loop(1, PLANE)
    def _(i):
        to = (p + i) % PLANE
        remote(left_in.at[to], left_out.at[p], sem_g.at[0], sem_g.at[1], plane_device(to, y))

    block_use(1)
    block_use(3)
    block_use(2)

    out_right = lft_m[pl.ds(RANK, RANK), pl.ds(pl.multiple_of(x * COLS, 128), COLS)].astype(f32)
    beside = jnp.concatenate([out_right] * 3 + [jnp.zeros((128 - 3 * RANK, COLS), f32)], axis=0)
    beside = beside.T.astype(bf16).reshape(NZ, NC, ROWS, 128)
    for b in range(NY):
        wbuf[b, :, :, :, pl.ds(COLS, 128)] = beside

    @pl.when(x != y)
    def _():
        local_wait(tgt.at[pl.ds(0, 128)], sem_t.at[7])

    tgt_t[...] = tgt[...].astype(f32).T

    wide.finish()
    acc[...] = -tgt_t[...]

    @pl.loop(0, NY)
    def _(b):
        rows = mt[b, pl.ds(0, 7)].reshape(COLS, tokens_n)
        low_o = noise_scale * jnp.dot(
            fb[b, pl.ds(RANK, RANK), pl.ds(0, COLS)], rows, preferred_element_type=f32
        )
        first = low_o.astype(bf16).astype(f32)
        second = (low_o - first).astype(bf16).astype(f32)
        third = low_o - first - second
        low_parts = jnp.concatenate(
            [first, second, third, jnp.zeros((128 - 3 * RANK, tokens_n), f32)], axis=0
        ).astype(bf16)
        term = jnp.dot(
            wbuf[b].reshape(COLS, COLS + 128),
            jnp.concatenate([rows, low_parts], axis=0),
            preferred_element_type=f32,
        )
        acc[...] += term.astype(bf16).astype(f32)

    part[x] = jnp.full((1, 128), jnp.sum(acc[...] * acc[...]), f32)
    for d in range(1, NX):
        remote(part.at[x], part.at[x], sem_e.at[0], sem_e.at[1], ((x + d) % NX, z, c, y))
    local_wait(fac_all.at[pl.ds(0, NX * NZ - 1), c], sem_f.at[1])
    remote(fac_all.at[:, c], fac_all.at[:, c], sem_f.at[2], sem_f.at[3], (x, z, 1 - c, y))
    local_wait(part.at[pl.ds(0, NX - 1)], sem_e.at[1])
    total[...] = part[0] + part[1] + part[2] + part[3]
    slot = (y * NZ + z) * NC + c
    ev[slot] = total[...]

    @pl.loop(1, PLANE)
    def _(i):
        to = (slot + i) % PLANE
        remote(
            total,
            ev.at[slot],
            sem_e.at[2],
            sem_e.at[3],
            (x, (to // NC) % NZ, to % NC, to // (NZ * NC)),
        )

    local_wait(left_out.at[pl.ds(0, PLANE - 1)], sem_g.at[1])
    local_wait(fac_all.at[:, 1 - c], sem_f.at[3])
    local_wait(ev.at[pl.ds(0, PLANE - 1)], sem_e.at[3])

    scored = -(ev[...].reshape(PLANE, 128) / (tokens_n * D))
    mean = jnp.sum(scored, axis=0, keepdims=True) / PLANE
    apart = scored - mean
    spread = jnp.sum(apart * apart, axis=0, keepdims=True) / PLANE
    weight = apart / jnp.sqrt(spread + spread_floor) / noise_scale
    fit[...] = -(ev[p] / (tokens_n * D))
    rank_at = lax.broadcasted_iota(jnp.int32, (PLANE, 8, 128), 1)
    left = left_out[...].astype(f32) * weight[:, None, :]
    left = jnp.concatenate(
        [
            jnp.where(rank_at < RANK, left, 0.0).reshape(PLANE * 8, 128),
            jnp.where(rank_at < RANK, 0.0, left).reshape(PLANE * 8, 128),
        ],
        axis=1,
    )
    right = fac_all[...].reshape(PLANE * 8, COLS)
    first = left.astype(bf16)
    rest = left - first.astype(f32)
    second = rest.astype(bf16)
    third = (rest - second.astype(f32)).astype(bf16)
    grads = jnp.zeros((256, COLS), f32)
    for piece in (third, second, first):
        grads += lax.dot_general(
            piece, right, (((0,), (0,)), ((), ())), preferred_element_type=f32
        )
    grad_q[...] = grads[:ROWS]
    grad_o[...] = grads[128 : 128 + ROWS]

    wide.drain()
    local_wait(slab_out.at[pl.ds(0, PLANE - 1)], sem_s.at[0])
    local_wait(left_out.at[pl.ds(0, PLANE - 1)], sem_g.at[0])

    @pl.when(x != y)
    def _():
        local_wait(lft_m, sem_t.at[0])
        local_wait(tgt.at[pl.ds(0, 128)], sem_t.at[6])
        local_wait(fb.at[:, :, pl.ds(0, COLS)], sem_t.at[4])

    @pl.when(x == y)
    def _():
        local_wait(tok.at[pl.ds(0, 3 * 128 * COLS // D)], sem_t.at[2])
        local_wait(fb.at[pl.ds(0, 3), :, pl.ds(0, COLS)], sem_t.at[4])

    local_wait(k4.at[pl.ds(0, 3), pl.ds(0, 128)], sem_k.at[0])
    local_wait(v4.at[pl.ds(0, 3), pl.ds(0, 64)], sem_k.at[2])
    local_wait(k4.at[:, pl.ds(0, 128)], sem_k.at[4])
    local_wait(v4.at[:, pl.ds(0, 64)], sem_k.at[7])
    local_wait(bt.at[pl.ds(0, 3), 0, 0, 0], sem_1.at[0])
    local_wait(bt.at[:, 0, pl.ds(0, 7), 0], sem_2.at[0])
    local_wait(bt.at[:, pl.ds(0, 3), :, 0], sem_3.at[0])
    local_wait(bt.at[:, :, :, 0], sem_4.at[0])
    local_wait(fac_all.at[pl.ds(0, NX * NZ - 1), c], sem_f.at[0])
    local_wait(fac_all.at[:, c], sem_f.at[2])
    local_wait(part.at[pl.ds(0, NX - 1)], sem_e.at[0])
    local_wait(ev.at[pl.ds(0, PLANE - 1)], sem_e.at[2])


def forward(ids, *ins):
    tok = ins[0].shape[0]
    bf16, f32 = jnp.bfloat16, jnp.float32
    held = [a for i, a in enumerate(ins) if i not in (3,)]
    order = (0, 1, 2, 3, 4, 5, 6, 7, 8, 9, 10)
    dma = pltpu.SemaphoreType.DMA
    return pl.pallas_call(
        forward_kernel,
        name="forward",
        out_shape=(
            jax.ShapeDtypeStruct((ROWS, COLS), f32),
            jax.ShapeDtypeStruct((ROWS, COLS), f32),
            jax.ShapeDtypeStruct((1, 128), f32),
        ),
        in_specs=[pl.BlockSpec(memory_space=pltpu.SMEM)]
        + [pl.BlockSpec(memory_space=pl.ANY)] * len(ins),
        out_specs=[pl.BlockSpec(memory_space=pltpu.VMEM)] * 3,
        scratch_shapes=[pltpu.VMEM(held[i].shape, held[i].dtype) for i in order]
        + [
            pltpu.VMEM((PLANE, SLAB, 128), bf16),
            pltpu.VMEM((PLANE, SLAB, 128), bf16),
            pltpu.VMEM((PLANE, 8, 128), bf16),
            pltpu.VMEM((PLANE, 8, 128), bf16),
            pltpu.VMEM((8, COLS), bf16),
            pltpu.VMEM((NX * NZ, NC, 8, COLS), bf16),
            pltpu.VMEM((8, D), bf16),
            pltpu.VMEM((PLANE, 1, 128), f32),
            pltpu.VMEM((NY, NZ, NC, ROWS, COLS + 128), bf16),
            pltpu.VMEM((NY, NX, NZ, NC, SLAB, tok), bf16),
            pltpu.VMEM((NY, 8, HEAD_DIM, tok), bf16),
            pltpu.VMEM((NY, tok, HEAD_DIM), bf16),
            pltpu.VMEM((NY, HEAD_DIM, tok), bf16),
            pltpu.VMEM((NY, 8, COLS + 128), bf16),
            pltpu.VMEM((8, D), bf16),
            pltpu.VMEM((COLS, tok), f32),
            pltpu.VMEM((COLS, tok), f32),
            pltpu.VMEM((8, tok), bf16),
            pltpu.VMEM((NX, 1, 128), f32),
            pltpu.VMEM((1, 128), f32),
            dma((12,)),
            dma((PlaneGather.SEMS,)),
            dma((2,)),
            dma((8,)),
            dma((8,)),
            dma((2,)),
            dma((8,)),
            dma((4,)),
            dma((5,)),
            dma((4,)),
            dma((4,)),
            dma((2,)),
        ],
        compiler_params=pltpu.CompilerParams(
            collective_id=0, has_side_effects=True, vmem_limit_bytes=60 * 1024 * 1024
        ),
    )(ids, *ins)


def tables(count, head_size):
    position = np.arange(count, dtype=np.float64)
    index = np.arange(head_size // 2, dtype=np.float64)
    freq = np.exp(-math.log(rope_base) * 2.0 * index / head_size)
    angle = freq[:, None] * position[None, :]
    return np.cos(angle).astype(np.float32), np.sin(angle).astype(np.float32)


def per_device(
    tokens,
    target,
    w_query,
    w_key,
    w_value,
    w_out,
    query_left_factors,
    query_right_factors,
    o_left,
    o_right,
    member_ids,
):
    cos_t, sin_t = tables(tokens.shape[0], HEAD_DIM)
    grad_q, grad_o, fit = forward(
        member_ids,
        tokens,
        w_key,
        w_value,
        jnp.transpose(w_out),
        target,
        w_query,
        jnp.transpose(query_left_factors[0]),
        query_right_factors[0],
        jnp.transpose(o_left[0]),
        o_right[0],
        cos_t,
        sin_t,
    )
    return (grad_q, jnp.transpose(grad_o), fit[0, :1])


def solution(mesh):
    torus = Mesh(mesh.devices.reshape(NX, NZ, NC, NY), AXES)
    placed = (
        P(),
        P(None, "mp"),
        P(POP, "mp"),
        P(None, "mp"),
        P(None, "mp"),
        P("mp", POP),
        P(POP, None, None),
        P(POP, None, "mp"),
        P(POP, "mp", None),
        P(POP, None, None),
        P(POP),
    )
    return jax.shard_map(
        per_device,
        mesh=torus,
        in_specs=placed,
        out_specs=(P(POP, "mp"), P("mp", POP), P(POP)),
        check_vma=False,
    )
```

```python
import math

import jax
import jax.numpy as jnp
import numpy as np
from jax import lax
from jax.experimental import pallas as pl
from jax.experimental.pallas import tpu as pltpu
from jax.sharding import Mesh
from jax.sharding import PartitionSpec as P

D = 3584
HEADS = 28
KV_HEADS = 4
HEAD_DIM = 128
RANK = 4
NX, NZ, NC, NY = 4, 8, 2, 4
PLANE = NX * NZ * NC
ROWS = D // PLANE
COLS = D // NY
AXES = ("pop_0", "pop_1", "pop_2", "mp")
POP = AXES[:3]
MESH = pl.DeviceIdType.MESH

noise_scale = 0.5
rope_base = 1000000.0
spread_floor = 0.001


def place():
    return tuple(lax.axis_index(a) for a in AXES)


PEERS = [(d, dz, dc) for d in (2, 1, 3, 0) for dz in (4, 3, 5, 2, 6, 1, 7, 0) for dc in (1, 0)]
PEERS.remove((0, 0, 0))


def local_wait(ref, sem):
    pltpu.make_async_copy(ref, ref, sem).wait()


class PlaneGather:
    SEMS = 49

    def __init__(self, me, buf, sem, cut):
        self.x, self.z, self.c, self.y = me
        self.sem = sem
        self.buf = buf
        self.a = pl.ds(0, cut)
        self.b = pl.ds(cut, COLS - cut)

    def zat(self, d):
        return (self.z + d + NZ) % NZ

    def yat(self, d):
        return (self.y + d + NY) % NY

    def send(self, ref, to, ssem, rsem):
        pltpu.make_async_remote_copy(
            src_ref=ref,
            dst_ref=ref,
            send_sem=self.sem.at[ssem],
            recv_sem=self.sem.at[rsem],
            device_id=to,
            device_id_type=MESH,
        ).start()

    def ydev(self, d):
        return (self.x, self.z, self.c, self.yat(d))

    def zdev(self, d):
        return (self.x, self.zat(d), self.c, self.y)

    def share(self, ref):
        self.send(ref, (self.x, self.z, 1 - self.c, self.y), 4, 5)

    def ra(self, right, s, h):
        return (7 if right else 15) + (s - 1) * 2 + h

    def rb(self, right, s):
        return (23 if right else 27) + s - 1

    def ry(self, right, k):
        return (31 if right else 39) + k

    @staticmethod
    def zoff(k):
        return -((k + 1) // 2) if k % 2 else k // 2

    def start(self):
        own_a = self.buf.at[self.y, self.z, self.c, :, self.a]
        own_b = self.buf.at[self.y, self.z, self.c, :, self.b]
        for d in (1, 3, 2):
            self.send(own_a, self.ydev(d), 0, 6)
        self.send(own_b, self.zdev(1), 2, self.rb(True, 1))
        self.send(own_b, self.zdev(-1), 2, self.rb(False, 1))
        self.send(own_b, self.ydev(1), 3, self.ry(True, 0))
        self.send(own_b, self.ydev(-1), 3, self.ry(False, 0))
        self.share(own_b)

    def a_line(self):
        local_wait(self.buf.at[pl.ds(0, 3), self.z, self.c, :, self.a], self.sem.at[6])
        for h in range(2):
            ref = self.buf.at[pl.ds(2 * h, 2), self.z, self.c, :, self.a]
            self.send(ref, self.zdev(1), 1, self.ra(True, 1, h))
            self.send(ref, self.zdev(-1), 1, self.ra(False, 1, h))
        self.share(self.buf.at[:, self.z, self.c, :, self.a])

    @staticmethod
    def a_moves(right, s, h):
        return s < 4 or (s == 4 and h == (0 if right else 1))

    def a_step(self, s):
        for h in range(2):
            for right in (True, False):
                if not self.a_moves(right, s, h):
                    continue
                zz = self.zat(-s if right else s)
                ref = self.buf.at[pl.ds(2 * h, 2), zz, self.c, :, self.a]
                local_wait(ref, self.sem.at[self.ra(right, s, h)])
                if s < 4 and self.a_moves(right, s + 1, h):
                    self.send(ref, self.zdev(1 if right else -1), 1, self.ra(right, s + 1, h))
                self.share(ref)

    def b_step(self, s):
        for right in (True, False):
            if s == 4 and not right:
                continue
            zz = self.zat(-s if right else s)
            k = 2 * s - 1 if right else 2 * s
            ref = self.buf.at[self.y, zz, self.c, :, self.b]
            local_wait(ref, self.sem.at[self.rb(right, s)])
            if s < 3 or (s == 3 and right):
                self.send(ref, self.zdev(1 if right else -1), 2, self.rb(right, s + 1))
            self.send(ref, self.ydev(1), 3, self.ry(True, k))
            self.send(ref, self.ydev(-1), 3, self.ry(False, k))
            self.share(ref)

    def y_step(self, k):
        zz = self.zat(self.zoff(k))
        for right in (True, False):
            ref = self.buf.at[self.yat(-1 if right else 1), zz, self.c, :, self.b]
            local_wait(ref, self.sem.at[self.ry(right, k)])
            if (k % 2 == 0) == right:
                self.send(ref, self.ydev(1 if right else -1), 3, 47 if right else 48)
            self.share(ref)

    def far(self):
        for s in (47, 48):
            local_wait(self.buf.at[0, pl.ds(0, 4), self.c, :, self.b], self.sem.at[s])
        self.share(self.buf.at[self.yat(2), :, self.c, :, self.b])

    def finish(self):
        local_wait(self.buf.at[:, :, 1 - self.c, :, pl.ds(0, COLS)], self.sem.at[5])

    def drain(self):
        local_wait(self.buf.at[pl.ds(0, 3), 0, 0, :, self.a], self.sem.at[0])
        local_wait(self.buf.at[:, pl.ds(0, 7), 0, :, self.a], self.sem.at[1])
        local_wait(self.buf.at[0, pl.ds(0, 7), 0, :, self.b], self.sem.at[2])
        local_wait(self.buf.at[pl.ds(0, 3), :, 0, :, self.b], self.sem.at[3])
        local_wait(self.buf.at[:, :, self.c, :, pl.ds(0, COLS)], self.sem.at[4])


CUT = 512
SLAB = 16


def remote(src, dst, ssem, rsem, to):
    pltpu.make_async_remote_copy(
        src_ref=src, dst_ref=dst, send_sem=ssem, recv_sem=rsem, device_id=to, device_id_type=MESH
    ).start()


def forward_kernel(
    ids, tok_h, wk_h, wv_h, wo_h, tgt_h, wq_h, ql_h, qr_h, ol_h, or_h, cos_h, sin_h,
    grad_q, grad_o, fit,
    tok, wk, wv, tgt, wq, ql, qr, ol, orr, cos, sin,
    slab_in, slab_out, left_in, left_out, fac, fac_all, lft, ev,
    wbuf, bt, mt, k4, v4, fb, lft_m, tgt_t, acc, low, part, total,
    sem_l, sem_w, sem_s, sem_t, sem_k, sem_1, sem_2, sem_3, sem_4, sem_f, sem_e, sem_g,
):
    me = place()
    x, z, c, y = me
    p = (x * NZ + z) * NC + c
    f32, bf16 = jnp.float32, jnp.bfloat16
    tokens_n = tok.shape[0]
    half = HEAD_DIM // 2
    sibling = (x, z, 1 - c, y)

    loads = {}
    for i, (name, src, dst) in enumerate(
        (
            ("wq", wq_h, wq),
            ("ql", ql_h, ql),
            ("or", or_h, orr),
            ("qr", qr_h, qr),
            ("ol", ol_h, ol),
            ("wo", wo_h, wbuf.at[y, z, c, :, pl.ds(0, COLS)]),
            ("tok", tok_h, tok),
            ("wk", wk_h, wk),
            ("wv", wv_h, wv),
            ("cos", cos_h, cos),
            ("sin", sin_h, sin),
            ("tgt", tgt_h, tgt),
        )
    ):
        loads[name] = pltpu.make_async_copy(src, dst, sem_l.at[i])
        loads[name].start()

    barrier = pltpu.get_barrier_semaphore()

    def greet(to):
        pl.semaphore_signal(barrier, inc=1, device_id=to, device_id_type=MESH)

    for dx, dz, dc in PEERS:
        greet(((x + dx) % NX, (z + dz) % NZ, (c + dc) % NC, y))

    for dy, dz, dc in PEERS:
        if dy:
            greet((x, (z + dz) % NZ, (c + dc) % NC, (y + dy) % NY))

    for dx in range(1, NX):
        for dy in range(1, NY):
            greet(((x + dx) % NX, z, c, (y + dy) % NY))

    def turned(v):
        first, second = v[:half], v[half:]
        ct, st = cos[...], sin[...]
        return jnp.concatenate([first * ct - second * st, second * ct + first * st], axis=0)

    sign = (1 - 2 * (ids[0] % 2)).astype(f32)
    for name in ("wq", "ql", "or", "qr", "ol"):
        loads[name].wait()
    slabs = wq[...].astype(f32).T.reshape(COLS // SLAB, 2, 8, ROWS).astype(bf16)
    for i in range(2):
        slab_in[pl.ds(0, COLS // SLAB), :, pl.ds(i * ROWS, ROWS)] = slabs[:, i]
    slab_in[pl.ds(COLS // SLAB, PLANE - COLS // SLAB)] = jnp.zeros(
        (PLANE - COLS // SLAB, 8, 128), bf16
    )
    fac[...] = jnp.concatenate([qr[...].astype(f32), ol[...].astype(f32)], axis=0).astype(bf16)
    lft[...] = (jnp.concatenate([ql[...].astype(f32), orr[...].astype(f32)], axis=0) * sign).astype(bf16)
    for i in range(PLANE):
        left_in[i, :, pl.ds(0, ROWS)] = lft[:, pl.ds(i * ROWS, ROWS)]
    fb[:, :, pl.ds(COLS, 128)] = jnp.zeros((NY, 8, 128), bf16)
    slab_out[p] = slab_in[p]
    left_out[p] = left_in[p]
    fac_all[x * NZ + z, c] = fac[...]

    for name in ("tok", "wk", "wv", "cos", "sin"):
        loads[name].wait()
    key_t = jnp.dot(tok[...], wk[...], preferred_element_type=f32).T
    k4[y] = turned(key_t).T.astype(bf16)
    v4[y] = jnp.dot(tok[...], wv[...], preferred_element_type=f32).T.astype(bf16)
    loads["wo"].wait()
    loads["tgt"].wait()
    pl.semaphore_wait(barrier, PLANE - 1 + 3 * NZ * NC + 9)

    def to_plane(src, dst, sem):
        for dx, dz, dc in PEERS:
            xx, zz, cc = (x + dx) % NX, (z + dz) % NZ, (c + dc) % NC
            remote(src.at[(xx * NZ + zz) * NC + cc], dst.at[p], sem.at[0], sem.at[1], (xx, zz, cc, y))

    to_plane(slab_in, slab_out, sem_s)

    @pl.when(x != y)
    def _():
        remote(lft, lft_m, sem_t.at[0], sem_t.at[1], (y, z, c, x))

    wide = PlaneGather(me, wbuf, sem_w, CUT)
    wide.start()

    key_half = k4.at[y, pl.ds(pl.multiple_of(c * 128, 128), 128)]
    value_half = v4.at[y, pl.ds(pl.multiple_of(c * 64, 64), 64)]
    for d in range(1, NY):
        to = (x, z, c, (y + d) % NY)
        remote(key_half, key_half, sem_k.at[0], sem_k.at[1], to)
        remote(value_half, value_half, sem_k.at[2], sem_k.at[3], to)

    @pl.when(x == y)
    def _():
        lft_m[...] = lft[...]

    @pl.when(x != y)
    def _():
        local_wait(lft_m, sem_t.at[1])

    local_wait(slab_out.at[pl.ds(0, PLANE - 1)], sem_s.at[1])
    made = lax.dot_general(
        jnp.concatenate(
            [
                jnp.concatenate(
                    [slab_out[i, :, pl.ds(h * ROWS, ROWS)] for i in range(PLANE)], axis=1
                )
                for h in range(2)
            ]
            + [lft_m[...]],
            axis=0,
        ),
        tok[...],
        (((1,), (1,)), ((), ())),
        preferred_element_type=f32,
    )
    bt[y, x, z, c] = made[:SLAB].astype(bf16)
    low[...] = made[SLAB : SLAB + 8].astype(bf16)
    mine = bt.at[y, x, z, c]
    for d in (4, 3, 5, 2, 6, 1, 7):
        remote(mine, mine, sem_1.at[0], sem_1.at[1], (x, (z + d) % NZ, c, y))

    wide.a_line()
    wide.b_step(1)
    wide.y_step(0)

    local_wait(bt.at[y, x, pl.ds(0, 7), c], sem_1.at[1])

    def line_out(yy):
        ref = bt.at[yy, x, :, c]
        for d in (1, 3, 2):
            remote(ref, ref, sem_3.at[0], sem_3.at[d], ((x + d) % NX, z, c, y))
        remote(ref, ref, sem_4.at[0], sem_4.at[1], sibling)

    line = bt.at[y, x, :, c]
    for d in (2, 1, 3):
        remote(line, line, sem_2.at[0], sem_2.at[d], (x, z, c, (y + d) % NY))
    line_out(y)

    tgt_half = tgt.at[pl.ds(pl.multiple_of(c * 128, 128), 128)]

    @pl.when(x == y)
    def _():
        for d in (2, 1, 3):
            to = (x, z, c, (y + d) % NY)
            remote(tgt_half, tgt_half, sem_t.at[2], sem_t.at[3], to)

    spot = fb.at[y, :, pl.ds(0, COLS)]

    @pl.when(x != y)
    def _():
        remote(fac, spot, sem_t.at[4], sem_t.at[5], (x, z, c, x))

    for d in range(1, NX):
        remote(fac, spot, sem_t.at[4], sem_t.at[5], ((x + d) % NX, z, c, x))

    @pl.when(x == y)
    def _():
        fb[y, :, pl.ds(0, COLS)] = fac[...]

    wide.a_step(1)
    wide.b_step(2)
    wide.y_step(1)
    wide.y_step(2)

    for d in (1, 3, 2):
        yy = (y + NY - d) % NY
        local_wait(bt.at[yy, x, :, c], sem_2.at[d])
        line_out(yy)

    wide.b_step(3)
    wide.a_step(2)
    wide.y_step(3)
    wide.y_step(4)

    local_wait(k4.at[pl.ds(0, 3), pl.ds(0, 128)], sem_k.at[1])
    keys_in = k4.at[:, pl.ds(pl.multiple_of(c * 128, 128), 128)]
    remote(keys_in, keys_in, sem_k.at[4], sem_k.at[5], sibling)
    local_wait(v4.at[pl.ds(0, 3), pl.ds(0, 64)], sem_k.at[3])
    values_in = v4.at[:, pl.ds(pl.multiple_of(c * 64, 64), 64)]
    remote(values_in, values_in, sem_k.at[7], sem_k.at[6], sibling)
    row = lax.broadcasted_iota(jnp.int32, (tokens_n, tokens_n), 0)
    col = lax.broadcasted_iota(jnp.int32, (tokens_n, tokens_n), 1)

    to_log2 = HEAD_DIM ** (-0.5) * math.log2(math.e)

    def attend(xb):
        @pl.loop(0, NY, step=2)
        def _(pair):
            for yh in (pair, pair + 1):
                right = fb[yh, pl.ds(0, RANK), pl.ds(pl.multiple_of(xb * 256, 256), 256)]
                shift = lax.dot_general(
                    right, low[pl.ds(0, RANK), :], (((0,), (0,)), ((), ())), preferred_element_type=f32
                )
                base = bt[yh, xb].reshape(2 * HEAD_DIM, tokens_n).astype(f32)
                query = base + noise_scale * shift
                for j in range(2):
                    q = turned(query[j * HEAD_DIM : (j + 1) * HEAD_DIM]).astype(bf16)
                    scores = jnp.dot(k4[yh], q, preferred_element_type=f32)
                    scores = jnp.where(row <= col, scores, -1e30)
                    scores = jnp.exp2((scores - jnp.max(scores, axis=0, keepdims=True)) * to_log2)
                    share = 1.0 / jnp.sum(scores, axis=0, keepdims=True)
                    mixed = jnp.dot(v4[yh], (scores * share).astype(bf16), preferred_element_type=f32)
                    mt[yh, xb * 2 + j] = mixed.astype(bf16)

    local_wait(bt.at[:, x, :, 1 - c], sem_4.at[1])
    local_wait(k4.at[:, pl.ds(0, 128)], sem_k.at[5])
    local_wait(v4.at[:, pl.ds(0, 64)], sem_k.at[6])

    @pl.when(x != y)
    def _():
        local_wait(fb.at[:, :, pl.ds(0, COLS)], sem_t.at[5])

    @pl.when(x == y)
    def _():
        local_wait(fb.at[pl.ds(0, 3), :, pl.ds(0, COLS)], sem_t.at[5])

    attend(x)
    wide.a_step(3)
    wide.b_step(4)
    wide.y_step(5)
    wide.y_step(6)

    def block_in(d):
        ref = bt.at[:, (x + NX - d) % NX, :, c]
        local_wait(ref, sem_3.at[d])
        remote(ref, ref, sem_4.at[0], sem_4.at[1 + d], sibling)

    def block_use(d):
        xb = (x + NX - d) % NX
        local_wait(bt.at[:, xb, :, 1 - c], sem_4.at[1 + d])
        attend(xb)

    block_in(1)
    block_in(3)

    block_use(1)
    wide.a_step(4)
    chip = x * NZ + z
    for d in range(1, NZ):
        remote(fac, fac_all.at[chip, c], sem_f.at[0], sem_f.at[1], (x, (z + d) % NZ, c, y))

    to_plane(left_in, left_out, sem_g)
    wide.y_step(7)
    block_in(2)
    block_use(3)
    wide.far()
    @pl.when(x != y)
    def _():
        local_wait(tgt_half, sem_t.at[3])
        remote(tgt_half, tgt_half, sem_t.at[6], sem_t.at[7], sibling)

    block_use(2)
    local_wait(fac_all.at[pl.ds(0, NZ - 1), c], sem_f.at[1])
    facs = fac_all.at[pl.ds(x * NZ, NZ), c]
    for d in range(1, NX):
        remote(facs, facs, sem_f.at[2], sem_f.at[3], ((x + d) % NX, z, c, y))

    out_right = lft_m[pl.ds(RANK, RANK), pl.ds(pl.multiple_of(x * COLS, 128), COLS)].astype(f32)
    beside = jnp.concatenate([out_right] * 3 + [jnp.zeros((128 - 3 * RANK, COLS), f32)], axis=0)
    beside = beside.T.astype(bf16).reshape(NZ, NC, ROWS, 128)
    for b in range(NY):
        wbuf[b, :, :, :, pl.ds(COLS, 128)] = beside

    @pl.when(x != y)
    def _():
        local_wait(tgt.at[pl.ds(0, 128)], sem_t.at[7])

    tgt_t[...] = tgt[...].astype(f32).T

    wide.finish()
    acc[...] = -tgt_t[...]

    @pl.loop(0, NY)
    def _(b):
        rows = mt[b, pl.ds(0, 7)].reshape(COLS, tokens_n)
        low_o = noise_scale * jnp.dot(
            fb[b, pl.ds(RANK, RANK), pl.ds(0, COLS)], rows, preferred_element_type=f32
        )
        first = low_o.astype(bf16).astype(f32)
        second = (low_o - first).astype(bf16).astype(f32)
        third = low_o - first - second
        low_parts = jnp.concatenate(
            [first, second, third, jnp.zeros((128 - 3 * RANK, tokens_n), f32)], axis=0
        ).astype(bf16)
        term = jnp.dot(
            wbuf[b].reshape(COLS, COLS + 128),
            jnp.concatenate([rows, low_parts], axis=0),
            preferred_element_type=f32,
        )
        acc[...] += term.astype(bf16).astype(f32)

    part[x] = jnp.full((1, 128), jnp.sum(acc[...] * acc[...]), f32)
    for d in range(1, NX):
        remote(part.at[x], part.at[x], sem_e.at[0], sem_e.at[1], ((x + d) % NX, z, c, y))
    local_wait(fac_all.at[pl.ds(0, 3 * NZ), c], sem_f.at[3])
    remote(fac_all.at[:, c], fac_all.at[:, c], sem_f.at[4], sem_f.at[5], sibling)
    local_wait(part.at[pl.ds(0, NX - 1)], sem_e.at[1])
    total[...] = part[0] + part[1] + part[2] + part[3]
    slot = (y * NZ + z) * NC + c
    ev[slot] = total[...]

    for dy, dz, dc in PEERS:
        to = (x, (z + dz) % NZ, (c + dc) % NC, (y + dy) % NY)
        remote(total, ev.at[slot], sem_e.at[2], sem_e.at[3], to)

    local_wait(left_out.at[pl.ds(0, PLANE - 1)], sem_g.at[1])
    local_wait(fac_all.at[:, 1 - c], sem_f.at[5])
    local_wait(ev.at[pl.ds(0, PLANE - 1)], sem_e.at[3])

    scored = -(ev[...].reshape(PLANE, 128) / (tokens_n * D))
    mean = jnp.sum(scored, axis=0, keepdims=True) / PLANE
    apart = scored - mean
    spread = jnp.sum(apart * apart, axis=0, keepdims=True) / PLANE
    weight = apart / jnp.sqrt(spread + spread_floor) / noise_scale
    fit[...] = -(ev[p] / (tokens_n * D))
    rank_at = lax.broadcasted_iota(jnp.int32, (PLANE, 8, 128), 1)
    left = left_out[...].astype(f32) * weight[:, None, :]
    left = jnp.concatenate(
        [
            jnp.where(rank_at < RANK, left, 0.0).reshape(PLANE * 8, 128),
            jnp.where(rank_at < RANK, 0.0, left).reshape(PLANE * 8, 128),
        ],
        axis=1,
    )
    right = fac_all[...].reshape(PLANE * 8, COLS)
    first = left.astype(bf16)
    rest = left - first.astype(f32)
    second = rest.astype(bf16)
    third = (rest - second.astype(f32)).astype(bf16)
    grads = jnp.zeros((256, COLS), f32)
    for piece in (third, second, first):
        grads += lax.dot_general(
            piece, right, (((0,), (0,)), ((), ())), preferred_element_type=f32
        )
    grad_q[...] = grads[:ROWS]
    grad_o[...] = grads[128 : 128 + ROWS]

    wide.drain()
    local_wait(slab_out.at[pl.ds(0, PLANE - 1)], sem_s.at[0])
    local_wait(left_out.at[pl.ds(0, PLANE - 1)], sem_g.at[0])

    @pl.when(x != y)
    def _():
        local_wait(lft_m, sem_t.at[0])
        local_wait(tgt.at[pl.ds(0, 128)], sem_t.at[6])
        local_wait(fb.at[:, :, pl.ds(0, COLS)], sem_t.at[4])

    @pl.when(x == y)
    def _():
        local_wait(tok.at[pl.ds(0, 3 * 128 * COLS // D)], sem_t.at[2])
        local_wait(fb.at[pl.ds(0, 3), :, pl.ds(0, COLS)], sem_t.at[4])

    local_wait(k4.at[pl.ds(0, 3), pl.ds(0, 128)], sem_k.at[0])
    local_wait(v4.at[pl.ds(0, 3), pl.ds(0, 64)], sem_k.at[2])
    local_wait(k4.at[:, pl.ds(0, 128)], sem_k.at[4])
    local_wait(v4.at[:, pl.ds(0, 64)], sem_k.at[7])
    local_wait(bt.at[0, 0, pl.ds(0, 7), 0], sem_1.at[0])
    local_wait(bt.at[pl.ds(0, 3), 0, :, 0], sem_2.at[0])
    local_wait(bt.at[:, pl.ds(0, 3), :, 0], sem_3.at[0])
    local_wait(bt.at[:, :, :, 0], sem_4.at[0])
    local_wait(fac_all.at[pl.ds(0, NZ - 1), c], sem_f.at[0])
    local_wait(fac_all.at[pl.ds(0, 3 * NZ), c], sem_f.at[2])
    local_wait(fac_all.at[:, c], sem_f.at[4])
    local_wait(part.at[pl.ds(0, NX - 1)], sem_e.at[0])
    local_wait(ev.at[pl.ds(0, PLANE - 1)], sem_e.at[2])


def forward(ids, *ins):
    tok = ins[0].shape[0]
    bf16, f32 = jnp.bfloat16, jnp.float32
    held = [a for i, a in enumerate(ins) if i not in (3,)]
    order = (0, 1, 2, 3, 4, 5, 6, 7, 8, 9, 10)
    dma = pltpu.SemaphoreType.DMA
    return pl.pallas_call(
        forward_kernel,
        name="forward",
        out_shape=(
            jax.ShapeDtypeStruct((ROWS, COLS), f32),
            jax.ShapeDtypeStruct((ROWS, COLS), f32),
            jax.ShapeDtypeStruct((1, 128), f32),
        ),
        in_specs=[pl.BlockSpec(memory_space=pltpu.SMEM)]
        + [pl.BlockSpec(memory_space=pl.ANY)] * len(ins),
        out_specs=[pl.BlockSpec(memory_space=pltpu.VMEM)] * 3,
        scratch_shapes=[pltpu.VMEM(held[i].shape, held[i].dtype) for i in order]
        + [
            pltpu.VMEM((PLANE, 8, 128), bf16),
            pltpu.VMEM((PLANE, 8, 128), bf16),
            pltpu.VMEM((PLANE, 8, 128), bf16),
            pltpu.VMEM((PLANE, 8, 128), bf16),
            pltpu.VMEM((8, COLS), bf16),
            pltpu.VMEM((NX * NZ, NC, 8, COLS), bf16),
            pltpu.VMEM((8, D), bf16),
            pltpu.VMEM((PLANE, 1, 128), f32),
            pltpu.VMEM((NY, NZ, NC, ROWS, COLS + 128), bf16),
            pltpu.VMEM((NY, NX, NZ, NC, SLAB, tok), bf16),
            pltpu.VMEM((NY, 8, HEAD_DIM, tok), bf16),
            pltpu.VMEM((NY, tok, HEAD_DIM), bf16),
            pltpu.VMEM((NY, HEAD_DIM, tok), bf16),
            pltpu.VMEM((NY, 8, COLS + 128), bf16),
            pltpu.VMEM((8, D), bf16),
            pltpu.VMEM((COLS, tok), f32),
            pltpu.VMEM((COLS, tok), f32),
            pltpu.VMEM((8, tok), bf16),
            pltpu.VMEM((NX, 1, 128), f32),
            pltpu.VMEM((1, 128), f32),
            dma((12,)),
            dma((PlaneGather.SEMS,)),
            dma((2,)),
            dma((8,)),
            dma((8,)),
            dma((2,)),
            dma((4,)),
            dma((4,)),
            dma((5,)),
            dma((6,)),
            dma((4,)),
            dma((2,)),
        ],
        compiler_params=pltpu.CompilerParams(
            collective_id=0, has_side_effects=True, vmem_limit_bytes=60 * 1024 * 1024
        ),
    )(ids, *ins)


def tables(count, head_size):
    position = np.arange(count, dtype=np.float64)
    index = np.arange(head_size // 2, dtype=np.float64)
    freq = np.exp(-math.log(rope_base) * 2.0 * index / head_size)
    angle = freq[:, None] * position[None, :]
    return np.cos(angle).astype(np.float32), np.sin(angle).astype(np.float32)


def per_device(
    tokens,
    target,
    w_query,
    w_key,
    w_value,
    w_out,
    query_left_factors,
    query_right_factors,
    o_left,
    o_right,
    member_ids,
):
    cos_t, sin_t = tables(tokens.shape[0], HEAD_DIM)
    grad_q, grad_o, fit = forward(
        member_ids,
        tokens,
        w_key,
        w_value,
        jnp.transpose(w_out),
        target,
        w_query,
        jnp.transpose(query_left_factors[0]),
        query_right_factors[0],
        jnp.transpose(o_left[0]),
        o_right[0],
        cos_t,
        sin_t,
    )
    return (grad_q, jnp.transpose(grad_o), fit[0, :1])


def solution(mesh):
    torus = Mesh(mesh.devices.reshape(NX, NZ, NC, NY), AXES)
    placed = (
        P(),
        P(None, "mp"),
        P(POP, "mp"),
        P(None, "mp"),
        P(None, "mp"),
        P("mp", POP),
        P(POP, None, None),
        P(POP, None, "mp"),
        P(POP, "mp", None),
        P(POP, None, None),
        P(POP),
    )
    return jax.shard_map(
        per_device,
        mesh=torus,
        in_specs=placed,
        out_specs=(P(POP, "mp"), P("mp", POP), P(POP)),
        check_vma=False,
    )
```

```python
import math

import jax
import jax.numpy as jnp
import numpy as np
from jax import lax
from jax.experimental import pallas as pl
from jax.experimental.pallas import tpu as pltpu
from jax.sharding import Mesh
from jax.sharding import PartitionSpec as P

D = 3584
HEADS = 28
KV_HEADS = 4
HEAD_DIM = 128
RANK = 4
NX, NZ, NC, NY = 4, 8, 2, 4
PLANE = NX * NZ * NC
ROWS = D // PLANE
COLS = D // NY
AXES = ("pop_0", "pop_1", "pop_2", "mp")
POP = AXES[:3]
MESH = pl.DeviceIdType.MESH

noise_scale = 0.5
rope_base = 1000000.0
spread_floor = 0.001


def place():
    return tuple(lax.axis_index(a) for a in AXES)


PEERS = [(d, dz, dc) for d in (2, 1, 3, 0) for dz in (4, 3, 5, 2, 6, 1, 7, 0) for dc in (1, 0)]
PEERS.remove((0, 0, 0))


def local_wait(ref, sem):
    pltpu.make_async_copy(ref, ref, sem).wait()


class PlaneGather:
    SEMS = 49

    def __init__(self, me, buf, sem, cut):
        self.x, self.z, self.c, self.y = me
        self.sem = sem
        self.buf = buf
        self.a = pl.ds(0, cut)
        self.b = pl.ds(cut, COLS - cut)

    def zat(self, d):
        return (self.z + d + NZ) % NZ

    def yat(self, d):
        return (self.y + d + NY) % NY

    def send(self, ref, to, ssem, rsem):
        pltpu.make_async_remote_copy(
            src_ref=ref,
            dst_ref=ref,
            send_sem=self.sem.at[ssem],
            recv_sem=self.sem.at[rsem],
            device_id=to,
            device_id_type=MESH,
        ).start()

    def ydev(self, d):
        return (self.x, self.z, self.c, self.yat(d))

    def zdev(self, d):
        return (self.x, self.zat(d), self.c, self.y)

    def share(self, ref):
        self.send(ref, (self.x, self.z, 1 - self.c, self.y), 4, 5)

    def ra(self, right, s, h):
        return (7 if right else 15) + (s - 1) * 2 + h

    def rb(self, right, s):
        return (23 if right else 27) + s - 1

    def ry(self, right, k):
        return (31 if right else 39) + k

    @staticmethod
    def zoff(k):
        return -((k + 1) // 2) if k % 2 else k // 2

    def start(self):
        own_a = self.buf.at[self.y, self.z, self.c, :, self.a]
        own_b = self.buf.at[self.y, self.z, self.c, :, self.b]
        for d in (1, 3, 2):
            self.send(own_a, self.ydev(d), 0, 6)
        self.send(own_b, self.zdev(1), 2, self.rb(True, 1))
        self.send(own_b, self.zdev(-1), 2, self.rb(False, 1))
        self.send(own_b, self.ydev(1), 3, self.ry(True, 0))
        self.send(own_b, self.ydev(-1), 3, self.ry(False, 0))
        self.share(own_b)

    def a_line(self):
        local_wait(self.buf.at[pl.ds(0, 3), self.z, self.c, :, self.a], self.sem.at[6])
        for h in range(2):
            ref = self.buf.at[pl.ds(2 * h, 2), self.z, self.c, :, self.a]
            self.send(ref, self.zdev(1), 1, self.ra(True, 1, h))
            self.send(ref, self.zdev(-1), 1, self.ra(False, 1, h))
        self.share(self.buf.at[:, self.z, self.c, :, self.a])

    @staticmethod
    def a_moves(right, s, h):
        return s < 4 or (s == 4 and h == (0 if right else 1))

    def a_step(self, s):
        for h in range(2):
            for right in (True, False):
                if not self.a_moves(right, s, h):
                    continue
                zz = self.zat(-s if right else s)
                ref = self.buf.at[pl.ds(2 * h, 2), zz, self.c, :, self.a]
                local_wait(ref, self.sem.at[self.ra(right, s, h)])
                if s < 4 and self.a_moves(right, s + 1, h):
                    self.send(ref, self.zdev(1 if right else -1), 1, self.ra(right, s + 1, h))
                self.share(ref)

    def b_step(self, s):
        for right in (True, False):
            if s == 4 and not right:
                continue
            zz = self.zat(-s if right else s)
            k = 2 * s - 1 if right else 2 * s
            ref = self.buf.at[self.y, zz, self.c, :, self.b]
            local_wait(ref, self.sem.at[self.rb(right, s)])
            if s < 3 or (s == 3 and right):
                self.send(ref, self.zdev(1 if right else -1), 2, self.rb(right, s + 1))
            self.send(ref, self.ydev(1), 3, self.ry(True, k))
            self.send(ref, self.ydev(-1), 3, self.ry(False, k))
            self.share(ref)

    def y_step(self, k):
        zz = self.zat(self.zoff(k))
        for right in (True, False):
            ref = self.buf.at[self.yat(-1 if right else 1), zz, self.c, :, self.b]
            local_wait(ref, self.sem.at[self.ry(right, k)])
            if (k % 2 == 0) == right:
                self.send(ref, self.ydev(1 if right else -1), 3, 47 if right else 48)
            self.share(ref)

    def far(self):
        for s in (47, 48):
            local_wait(self.buf.at[0, pl.ds(0, 4), self.c, :, self.b], self.sem.at[s])
        self.share(self.buf.at[self.yat(2), :, self.c, :, self.b])

    def finish(self):
        local_wait(self.buf.at[:, :, 1 - self.c, :, pl.ds(0, COLS)], self.sem.at[5])

    def drain(self):
        local_wait(self.buf.at[pl.ds(0, 3), 0, 0, :, self.a], self.sem.at[0])
        local_wait(self.buf.at[:, pl.ds(0, 7), 0, :, self.a], self.sem.at[1])
        local_wait(self.buf.at[0, pl.ds(0, 7), 0, :, self.b], self.sem.at[2])
        local_wait(self.buf.at[pl.ds(0, 3), :, 0, :, self.b], self.sem.at[3])
        local_wait(self.buf.at[:, :, self.c, :, pl.ds(0, COLS)], self.sem.at[4])


CUT = 512
SLAB = 16


def remote(src, dst, ssem, rsem, to):
    pltpu.make_async_remote_copy(
        src_ref=src, dst_ref=dst, send_sem=ssem, recv_sem=rsem, device_id=to, device_id_type=MESH
    ).start()


def forward_kernel(
    ids_h, tok_h, wk_h, wv_h, wo_h, tgt_h, wq_h, ql_h, qr_h, ol_h, or_h, cos_h, sin_h,
    grad_q, grad_o, fit,
    tok, wk, wv, tgt, wq, ql, qr, ol, orr, cos, sin,
    slab_in, slab_out, left_in, left_out, fac, fac_all, lft, ev,
    ids, wbuf, bt, mt, k4, v4, fb, lft_m, tgt_t, acc, low, part, total,
    sem_l, sem_w, sem_s, sem_t, sem_k, sem_1, sem_2, sem_3, sem_4, sem_f, sem_e, sem_g,
):
    me = place()
    x, z, c, y = me
    p = (x * NZ + z) * NC + c
    f32, bf16 = jnp.float32, jnp.bfloat16
    tokens_n = tok.shape[0]
    half = HEAD_DIM // 2
    sibling = (x, z, 1 - c, y)

    loads = {}
    for i, (name, src, dst) in enumerate(
        (
            ("wq", wq_h, wq),
            ("ql", ql_h, ql),
            ("or", or_h, orr),
            ("qr", qr_h, qr),
            ("ol", ol_h, ol),
            ("wo", wo_h, wbuf.at[y, z, c, :, pl.ds(0, COLS)]),
            ("tok", tok_h, tok),
            ("wk", wk_h, wk),
            ("wv", wv_h, wv),
            ("cos", cos_h, cos),
            ("sin", sin_h, sin),
            ("tgt", tgt_h, tgt),
            ("ids", ids_h, ids),
        )
    ):
        loads[name] = pltpu.make_async_copy(src, dst, sem_l.at[i])
        loads[name].start()

    barrier = pltpu.get_barrier_semaphore()

    def greet(to):
        pl.semaphore_signal(barrier, inc=1, device_id=to, device_id_type=MESH)

    for dx, dz, dc in PEERS:
        greet(((x + dx) % NX, (z + dz) % NZ, (c + dc) % NC, y))

    for dy, dz, dc in PEERS:
        if dy:
            greet((x, (z + dz) % NZ, (c + dc) % NC, (y + dy) % NY))

    for dx in range(1, NX):
        for dy in range(1, NY):
            greet(((x + dx) % NX, z, c, (y + dy) % NY))

    def turned(v):
        first, second = v[:half], v[half:]
        ct, st = cos[...], sin[...]
        return jnp.concatenate([first * ct - second * st, second * ct + first * st], axis=0)

    for name in ("ids", "wq", "ql", "or", "qr", "ol"):
        loads[name].wait()
    sign = (1 - 2 * (ids[...].reshape(1, 1) % 2)).astype(f32)
    slabs = wq[...].astype(f32).T.reshape(COLS // SLAB, 2, 8, ROWS).astype(bf16)
    for i in range(2):
        slab_in[pl.ds(0, COLS // SLAB), :, pl.ds(i * ROWS, ROWS)] = slabs[:, i]
    slab_in[pl.ds(COLS // SLAB, PLANE - COLS // SLAB)] = jnp.zeros(
        (PLANE - COLS // SLAB, 8, 128), bf16
    )
    fac[...] = jnp.concatenate([qr[...].astype(f32), ol[...].astype(f32)], axis=0).astype(bf16)
    lft[...] = (jnp.concatenate([ql[...].astype(f32), orr[...].astype(f32)], axis=0) * sign).astype(bf16)
    for i in range(PLANE):
        left_in[i, :, pl.ds(0, ROWS)] = lft[:, pl.ds(i * ROWS, ROWS)]
    fb[:, :, pl.ds(COLS, 128)] = jnp.zeros((NY, 8, 128), bf16)
    slab_out[p] = slab_in[p]
    left_out[p] = left_in[p]
    fac_all[x * NZ + z, c] = fac[...]

    for name in ("tok", "wk", "wv", "cos", "sin"):
        loads[name].wait()
    key_t = jnp.dot(tok[...], wk[...], preferred_element_type=f32).T
    k4[y] = turned(key_t).T.astype(bf16)
    v4[y] = jnp.dot(tok[...], wv[...], preferred_element_type=f32).T.astype(bf16)
    loads["wo"].wait()
    loads["tgt"].wait()
    pl.semaphore_wait(barrier, PLANE - 1 + 3 * NZ * NC + 9)

    def to_plane(src, dst, sem):
        for dx, dz, dc in PEERS:
            xx, zz, cc = (x + dx) % NX, (z + dz) % NZ, (c + dc) % NC
            remote(src.at[(xx * NZ + zz) * NC + cc], dst.at[p], sem.at[0], sem.at[1], (xx, zz, cc, y))

    to_plane(slab_in, slab_out, sem_s)

    @pl.when(x != y)
    def _():
        remote(lft, lft_m, sem_t.at[0], sem_t.at[1], (y, z, c, x))

    wide = PlaneGather(me, wbuf, sem_w, CUT)
    wide.start()

    key_half = k4.at[y, pl.ds(pl.multiple_of(c * 128, 128), 128)]
    value_half = v4.at[y, pl.ds(pl.multiple_of(c * 64, 64), 64)]
    for d in range(1, NY):
        to = (x, z, c, (y + d) % NY)
        remote(key_half, key_half, sem_k.at[0], sem_k.at[1], to)
        remote(value_half, value_half, sem_k.at[2], sem_k.at[3], to)

    @pl.when(x == y)
    def _():
        lft_m[...] = lft[...]

    @pl.when(x != y)
    def _():
        local_wait(lft_m, sem_t.at[1])

    local_wait(slab_out.at[pl.ds(0, PLANE - 1)], sem_s.at[1])
    made = lax.dot_general(
        jnp.concatenate(
            [
                jnp.concatenate(
                    [slab_out[i, :, pl.ds(h * ROWS, ROWS)] for i in range(PLANE)], axis=1
                )
                for h in range(2)
            ]
            + [lft_m[...]],
            axis=0,
        ),
        tok[...],
        (((1,), (1,)), ((), ())),
        preferred_element_type=f32,
    )
    bt[y, x, z, c] = made[:SLAB].astype(bf16)
    low[...] = made[SLAB : SLAB + 8].astype(bf16)
    mine = bt.at[y, x, z, c]
    for d in (4, 3, 5, 2, 6, 1, 7):
        remote(mine, mine, sem_1.at[0], sem_1.at[1], (x, (z + d) % NZ, c, y))

    wide.a_line()
    wide.b_step(1)
    wide.y_step(0)

    local_wait(bt.at[y, x, pl.ds(0, 7), c], sem_1.at[1])

    def line_out(yy):
        ref = bt.at[yy, x, :, c]
        for d in (1, 3, 2):
            remote(ref, ref, sem_3.at[0], sem_3.at[d], ((x + d) % NX, z, c, y))
        remote(ref, ref, sem_4.at[0], sem_4.at[1], sibling)

    line = bt.at[y, x, :, c]
    for d in (2, 1, 3):
        remote(line, line, sem_2.at[0], sem_2.at[d], (x, z, c, (y + d) % NY))
    line_out(y)

    tgt_half = tgt.at[pl.ds(pl.multiple_of(c * 128, 128), 128)]

    @pl.when(x == y)
    def _():
        for d in (2, 1, 3):
            to = (x, z, c, (y + d) % NY)
            remote(tgt_half, tgt_half, sem_t.at[2], sem_t.at[3], to)

    spot = fb.at[y, :, pl.ds(0, COLS)]

    @pl.when(x != y)
    def _():
        remote(fac, spot, sem_t.at[4], sem_t.at[5], (x, z, c, x))

    for d in range(1, NX):
        remote(fac, spot, sem_t.at[4], sem_t.at[5], ((x + d) % NX, z, c, x))

    @pl.when(x == y)
    def _():
        fb[y, :, pl.ds(0, COLS)] = fac[...]

    local_wait(k4.at[pl.ds(0, 3), pl.ds(0, 128)], sem_k.at[1])
    keys_in = k4.at[:, pl.ds(pl.multiple_of(c * 128, 128), 128)]
    remote(keys_in, keys_in, sem_k.at[4], sem_k.at[5], sibling)
    local_wait(v4.at[pl.ds(0, 3), pl.ds(0, 64)], sem_k.at[3])
    values_in = v4.at[:, pl.ds(pl.multiple_of(c * 64, 64), 64)]
    remote(values_in, values_in, sem_k.at[7], sem_k.at[6], sibling)
    for d in (1, 3, 2):
        yy = (y + NY - d) % NY
        local_wait(bt.at[yy, x, :, c], sem_2.at[d])
        line_out(yy)

    wide.a_step(1)
    wide.b_step(2)
    wide.y_step(1)
    wide.y_step(2)

    row = lax.broadcasted_iota(jnp.int32, (tokens_n, tokens_n), 0)
    col = lax.broadcasted_iota(jnp.int32, (tokens_n, tokens_n), 1)

    to_log2 = HEAD_DIM ** (-0.5) * math.log2(math.e)

    def attend(xb):
        @pl.loop(0, NY, step=2)
        def _(pair):
            for yh in (pair, pair + 1):
                right = fb[yh, pl.ds(0, RANK), pl.ds(pl.multiple_of(xb * 256, 256), 256)]
                shift = lax.dot_general(
                    right, low[pl.ds(0, RANK), :], (((0,), (0,)), ((), ())), preferred_element_type=f32
                )
                base = bt[yh, xb].reshape(2 * HEAD_DIM, tokens_n).astype(f32)
                query = base + noise_scale * shift
                for j in range(2):
                    q = turned(query[j * HEAD_DIM : (j + 1) * HEAD_DIM]).astype(bf16)
                    scores = jnp.dot(k4[yh], q, preferred_element_type=f32)
                    scores = jnp.where(row <= col, scores, -1e30)
                    scores = jnp.exp2((scores - jnp.max(scores, axis=0, keepdims=True)) * to_log2)
                    share = 1.0 / jnp.sum(scores, axis=0, keepdims=True)
                    mixed = jnp.dot(v4[yh], (scores * share).astype(bf16), preferred_element_type=f32)
                    mt[yh, xb * 2 + j] = mixed.astype(bf16)

    local_wait(bt.at[:, x, :, 1 - c], sem_4.at[1])
    local_wait(k4.at[:, pl.ds(0, 128)], sem_k.at[5])
    local_wait(v4.at[:, pl.ds(0, 64)], sem_k.at[6])

    @pl.when(x != y)
    def _():
        local_wait(fb.at[:, :, pl.ds(0, COLS)], sem_t.at[5])

    @pl.when(x == y)
    def _():
        local_wait(fb.at[pl.ds(0, 3), :, pl.ds(0, COLS)], sem_t.at[5])

    attend(x)
    wide.b_step(3)
    wide.a_step(2)
    wide.y_step(3)
    wide.y_step(4)

    chip = x * NZ + z
    for d in range(1, NZ):
        remote(fac, fac_all.at[chip, c], sem_f.at[0], sem_f.at[1], (x, (z + d) % NZ, c, y))


    def block_in(d):
        ref = bt.at[:, (x + NX - d) % NX, :, c]
        local_wait(ref, sem_3.at[d])
        remote(ref, ref, sem_4.at[0], sem_4.at[1 + d], sibling)

    def block_use(d):
        xb = (x + NX - d) % NX
        local_wait(bt.at[:, xb, :, 1 - c], sem_4.at[1 + d])
        attend(xb)

    block_in(1)
    block_in(3)

    block_use(1)
    wide.a_step(3)
    wide.b_step(4)
    wide.y_step(5)
    wide.y_step(6)
    block_in(2)
    block_use(3)
    wide.a_step(4)
    wide.y_step(7)

    to_plane(left_in, left_out, sem_g)

    @pl.when(x != y)
    def _():
        local_wait(tgt_half, sem_t.at[3])
        remote(tgt_half, tgt_half, sem_t.at[6], sem_t.at[7], sibling)

    block_use(2)
    wide.far()
    local_wait(fac_all.at[pl.ds(0, NZ - 1), c], sem_f.at[1])
    facs = fac_all.at[pl.ds(x * NZ, NZ), c]
    for d in range(1, NX):
        remote(facs, facs, sem_f.at[2], sem_f.at[3], ((x + d) % NX, z, c, y))

    out_right = lft_m[pl.ds(RANK, RANK), pl.ds(pl.multiple_of(x * COLS, 128), COLS)].astype(f32)
    beside = jnp.concatenate([out_right] * 3 + [jnp.zeros((128 - 3 * RANK, COLS), f32)], axis=0)
    beside = beside.T.astype(bf16).reshape(NZ, NC, ROWS, 128)
    for b in range(NY):
        wbuf[b, :, :, :, pl.ds(COLS, 128)] = beside

    @pl.when(x != y)
    def _():
        local_wait(tgt.at[pl.ds(0, 128)], sem_t.at[7])

    tgt_t[...] = tgt[...].astype(f32).T

    wide.finish()
    acc[...] = -tgt_t[...]

    @pl.loop(0, NY)
    def _(b):
        rows = mt[b, pl.ds(0, 7)].reshape(COLS, tokens_n)
        low_o = noise_scale * jnp.dot(
            fb[b, pl.ds(RANK, RANK), pl.ds(0, COLS)], rows, preferred_element_type=f32
        )
        first = low_o.astype(bf16).astype(f32)
        second = (low_o - first).astype(bf16).astype(f32)
        third = low_o - first - second
        low_parts = jnp.concatenate(
            [first, second, third, jnp.zeros((128 - 3 * RANK, tokens_n), f32)], axis=0
        ).astype(bf16)
        term = jnp.dot(
            wbuf[b].reshape(COLS, COLS + 128),
            jnp.concatenate([rows, low_parts], axis=0),
            preferred_element_type=f32,
        )
        acc[...] += term.astype(bf16).astype(f32)

    part[x] = jnp.full((1, 128), jnp.sum(acc[...] * acc[...]), f32)
    for d in range(1, NX):
        remote(part.at[x], part.at[x], sem_e.at[0], sem_e.at[1], ((x + d) % NX, z, c, y))
    local_wait(fac_all.at[pl.ds(0, 3 * NZ), c], sem_f.at[3])
    remote(fac_all.at[:, c], fac_all.at[:, c], sem_f.at[4], sem_f.at[5], sibling)
    local_wait(part.at[pl.ds(0, NX - 1)], sem_e.at[1])
    total[...] = part[0] + part[1] + part[2] + part[3]
    slot = (y * NZ + z) * NC + c
    ev[slot] = total[...]

    for dy, dz, dc in PEERS:
        to = (x, (z + dz) % NZ, (c + dc) % NC, (y + dy) % NY)
        remote(total, ev.at[slot], sem_e.at[2], sem_e.at[3], to)

    local_wait(left_out.at[pl.ds(0, PLANE - 1)], sem_g.at[1])
    local_wait(fac_all.at[:, 1 - c], sem_f.at[5])
    local_wait(ev.at[pl.ds(0, PLANE - 1)], sem_e.at[3])

    scored = -(ev[...].reshape(PLANE, 128) / (tokens_n * D))
    mean = jnp.sum(scored, axis=0, keepdims=True) / PLANE
    apart = scored - mean
    spread = jnp.sum(apart * apart, axis=0, keepdims=True) / PLANE
    weight = apart / jnp.sqrt(spread + spread_floor) / noise_scale
    fit[...] = -(ev[p] / (tokens_n * D))
    rank_at = lax.broadcasted_iota(jnp.int32, (PLANE, 8, 128), 1)
    left = left_out[...].astype(f32) * weight[:, None, :]
    left = jnp.concatenate(
        [
            jnp.where(rank_at < RANK, left, 0.0).reshape(PLANE * 8, 128),
            jnp.where(rank_at < RANK, 0.0, left).reshape(PLANE * 8, 128),
        ],
        axis=1,
    )
    right = fac_all[...].reshape(PLANE * 8, COLS)
    first = left.astype(bf16)
    rest = left - first.astype(f32)
    second = rest.astype(bf16)
    third = (rest - second.astype(f32)).astype(bf16)
    grads = jnp.zeros((256, COLS), f32)
    for piece in (third, second, first):
        grads += lax.dot_general(
            piece, right, (((0,), (0,)), ((), ())), preferred_element_type=f32
        )
    grad_q[...] = grads[:ROWS]
    grad_o[...] = grads[128 : 128 + ROWS]

    wide.drain()
    local_wait(slab_out.at[pl.ds(0, PLANE - 1)], sem_s.at[0])
    local_wait(left_out.at[pl.ds(0, PLANE - 1)], sem_g.at[0])

    @pl.when(x != y)
    def _():
        local_wait(lft_m, sem_t.at[0])
        local_wait(tgt.at[pl.ds(0, 128)], sem_t.at[6])
        local_wait(fb.at[:, :, pl.ds(0, COLS)], sem_t.at[4])

    @pl.when(x == y)
    def _():
        local_wait(tok.at[pl.ds(0, 3 * 128 * COLS // D)], sem_t.at[2])
        local_wait(fb.at[pl.ds(0, 3), :, pl.ds(0, COLS)], sem_t.at[4])

    local_wait(k4.at[pl.ds(0, 3), pl.ds(0, 128)], sem_k.at[0])
    local_wait(v4.at[pl.ds(0, 3), pl.ds(0, 64)], sem_k.at[2])
    local_wait(k4.at[:, pl.ds(0, 128)], sem_k.at[4])
    local_wait(v4.at[:, pl.ds(0, 64)], sem_k.at[7])
    local_wait(bt.at[0, 0, pl.ds(0, 7), 0], sem_1.at[0])
    local_wait(bt.at[pl.ds(0, 3), 0, :, 0], sem_2.at[0])
    local_wait(bt.at[:, pl.ds(0, 3), :, 0], sem_3.at[0])
    local_wait(bt.at[:, :, :, 0], sem_4.at[0])
    local_wait(fac_all.at[pl.ds(0, NZ - 1), c], sem_f.at[0])
    local_wait(fac_all.at[pl.ds(0, 3 * NZ), c], sem_f.at[2])
    local_wait(fac_all.at[:, c], sem_f.at[4])
    local_wait(part.at[pl.ds(0, NX - 1)], sem_e.at[0])
    local_wait(ev.at[pl.ds(0, PLANE - 1)], sem_e.at[2])


def forward(ids, *ins):
    tok = ins[0].shape[0]
    bf16, f32 = jnp.bfloat16, jnp.float32
    held = [a for i, a in enumerate(ins) if i not in (3,)]
    order = (0, 1, 2, 3, 4, 5, 6, 7, 8, 9, 10)
    dma = pltpu.SemaphoreType.DMA
    return pl.pallas_call(
        forward_kernel,
        name="forward",
        out_shape=(
            jax.ShapeDtypeStruct((ROWS, COLS), f32),
            jax.ShapeDtypeStruct((ROWS, COLS), f32),
            jax.ShapeDtypeStruct((1, 128), f32),
        ),
        in_specs=[pl.BlockSpec(memory_space=pl.ANY)] * (1 + len(ins)),
        out_specs=[pl.BlockSpec(memory_space=pltpu.VMEM)] * 3,
        scratch_shapes=[pltpu.VMEM(held[i].shape, held[i].dtype) for i in order]
        + [
            pltpu.VMEM((PLANE, 8, 128), bf16),
            pltpu.VMEM((PLANE, 8, 128), bf16),
            pltpu.VMEM((PLANE, 8, 128), bf16),
            pltpu.VMEM((PLANE, 8, 128), bf16),
            pltpu.VMEM((8, COLS), bf16),
            pltpu.VMEM((NX * NZ, NC, 8, COLS), bf16),
            pltpu.VMEM((8, D), bf16),
            pltpu.VMEM((PLANE, 1, 128), f32),
            pltpu.VMEM((1,), jnp.int32),
            pltpu.VMEM((NY, NZ, NC, ROWS, COLS + 128), bf16),
            pltpu.VMEM((NY, NX, NZ, NC, SLAB, tok), bf16),
            pltpu.VMEM((NY, 8, HEAD_DIM, tok), bf16),
            pltpu.VMEM((NY, tok, HEAD_DIM), bf16),
            pltpu.VMEM((NY, HEAD_DIM, tok), bf16),
            pltpu.VMEM((NY, 8, COLS + 128), bf16),
            pltpu.VMEM((8, D), bf16),
            pltpu.VMEM((COLS, tok), f32),
            pltpu.VMEM((COLS, tok), f32),
            pltpu.VMEM((8, tok), bf16),
            pltpu.VMEM((NX, 1, 128), f32),
            pltpu.VMEM((1, 128), f32),
            dma((13,)),
            dma((PlaneGather.SEMS,)),
            dma((2,)),
            dma((8,)),
            dma((8,)),
            dma((2,)),
            dma((4,)),
            dma((4,)),
            dma((5,)),
            dma((6,)),
            dma((4,)),
            dma((2,)),
        ],
        compiler_params=pltpu.CompilerParams(
            collective_id=0, has_side_effects=True, vmem_limit_bytes=60 * 1024 * 1024
        ),
    )(ids, *ins)


def hand_on(*arrays):
    def body(*refs):
        for i in range(len(arrays)):
            refs[len(arrays) + i][...] = refs[i][...]

    return pl.pallas_call(
        body,
        name="hand_on",
        out_shape=[jax.ShapeDtypeStruct(a.shape, a.dtype) for a in arrays],
        in_specs=[pl.BlockSpec(memory_space=pltpu.VMEM)] * len(arrays),
        out_specs=[pl.BlockSpec(memory_space=pltpu.VMEM)] * len(arrays),
    )(*arrays)


def tables(count, head_size):
    position = np.arange(count, dtype=np.float64)
    index = np.arange(head_size // 2, dtype=np.float64)
    freq = np.exp(-math.log(rope_base) * 2.0 * index / head_size)
    angle = freq[:, None] * position[None, :]
    return np.cos(angle).astype(np.float32), np.sin(angle).astype(np.float32)


def per_device(
    tokens,
    target,
    w_query,
    w_key,
    w_value,
    w_out,
    query_left_factors,
    query_right_factors,
    o_left,
    o_right,
    member_ids,
):
    cos_t, sin_t = tables(tokens.shape[0], HEAD_DIM)
    grad_q, grad_o, fit = forward(
        member_ids,
        tokens,
        w_key,
        w_value,
        jnp.transpose(w_out),
        target,
        w_query,
        jnp.transpose(query_left_factors[0]),
        query_right_factors[0],
        jnp.transpose(o_left[0]),
        o_right[0],
        cos_t,
        sin_t,
    )
    grad_q, grad_o, fit = hand_on(grad_q, grad_o, fit)
    return (grad_q, jnp.transpose(grad_o), fit[0, :1])


def solution(mesh):
    torus = Mesh(mesh.devices.reshape(NX, NZ, NC, NY), AXES)
    placed = (
        P(),
        P(None, "mp"),
        P(POP, "mp"),
        P(None, "mp"),
        P(None, "mp"),
        P("mp", POP),
        P(POP, None, None),
        P(POP, None, "mp"),
        P(POP, "mp", None),
        P(POP, None, None),
        P(POP),
    )
    return jax.shard_map(
        per_device,
        mesh=torus,
        in_specs=placed,
        out_specs=(P(POP, "mp"), P("mp", POP), P(POP)),
        check_vma=False,
    )
```

```python
import math

import jax
import jax.numpy as jnp
import numpy as np
from jax import lax
from jax.experimental import pallas as pl
from jax.experimental.pallas import tpu as pltpu
from jax.sharding import Mesh
from jax.sharding import PartitionSpec as P

D = 3584
HEADS = 28
KV_HEADS = 4
HEAD_DIM = 128
RANK = 4
NX, NZ, NC, NY = 4, 8, 2, 4
PLANE = NX * NZ * NC
ROWS = D // PLANE
COLS = D // NY
AXES = ("pop_0", "pop_1", "pop_2", "mp")
POP = AXES[:3]
MESH = pl.DeviceIdType.MESH

noise_scale = 0.5
rope_base = 1000000.0
spread_floor = 0.001


def place():
    return tuple(lax.axis_index(a) for a in AXES)


PEERS = [(d, dz, dc) for d in (2, 1, 3, 0) for dz in (4, 3, 5, 2, 6, 1, 7, 0) for dc in (1, 0)]
PEERS.remove((0, 0, 0))


def local_wait(ref, sem):
    pltpu.make_async_copy(ref, ref, sem).wait()


class PlaneGather:
    SEMS = 49

    def __init__(self, me, buf, sem, cut):
        self.x, self.z, self.c, self.y = me
        self.sem = sem
        self.buf = buf
        self.a = pl.ds(0, cut)
        self.b = pl.ds(cut, COLS - cut)

    def zat(self, d):
        return (self.z + d + NZ) % NZ

    def yat(self, d):
        return (self.y + d + NY) % NY

    def send(self, ref, to, ssem, rsem):
        pltpu.make_async_remote_copy(
            src_ref=ref,
            dst_ref=ref,
            send_sem=self.sem.at[ssem],
            recv_sem=self.sem.at[rsem],
            device_id=to,
            device_id_type=MESH,
        ).start()

    def ydev(self, d):
        return (self.x, self.z, self.c, self.yat(d))

    def zdev(self, d):
        return (self.x, self.zat(d), self.c, self.y)

    def share(self, ref):
        self.send(ref, (self.x, self.z, 1 - self.c, self.y), 4, 5)

    def ra(self, right, s, h):
        return (7 if right else 15) + (s - 1) * 2 + h

    def rb(self, right, s):
        return (23 if right else 27) + s - 1

    def ry(self, right, k):
        return (31 if right else 39) + k

    @staticmethod
    def zoff(k):
        return -((k + 1) // 2) if k % 2 else k // 2

    def start(self):
        own_a = self.buf.at[self.y, self.z, self.c, :, self.a]
        own_b = self.buf.at[self.y, self.z, self.c, :, self.b]
        for d in (1, 3, 2):
            self.send(own_a, self.ydev(d), 0, 6)
        self.send(own_b, self.zdev(1), 2, self.rb(True, 1))
        self.send(own_b, self.zdev(-1), 2, self.rb(False, 1))
        self.send(own_b, self.ydev(1), 3, self.ry(True, 0))
        self.send(own_b, self.ydev(-1), 3, self.ry(False, 0))
        self.share(own_b)

    def a_line(self):
        local_wait(self.buf.at[pl.ds(0, 3), self.z, self.c, :, self.a], self.sem.at[6])
        for h in range(2):
            ref = self.buf.at[pl.ds(2 * h, 2), self.z, self.c, :, self.a]
            self.send(ref, self.zdev(1), 1, self.ra(True, 1, h))
            self.send(ref, self.zdev(-1), 1, self.ra(False, 1, h))
        self.share(self.buf.at[:, self.z, self.c, :, self.a])

    @staticmethod
    def a_moves(right, s, h):
        return s < 4 or (s == 4 and h == (0 if right else 1))

    def a_step(self, s):
        for h in range(2):
            for right in (True, False):
                if not self.a_moves(right, s, h):
                    continue
                zz = self.zat(-s if right else s)
                ref = self.buf.at[pl.ds(2 * h, 2), zz, self.c, :, self.a]
                local_wait(ref, self.sem.at[self.ra(right, s, h)])
                if s < 4 and self.a_moves(right, s + 1, h):
                    self.send(ref, self.zdev(1 if right else -1), 1, self.ra(right, s + 1, h))
                self.share(ref)

    def b_step(self, s):
        for right in (True, False):
            if s == 4 and not right:
                continue
            zz = self.zat(-s if right else s)
            k = 2 * s - 1 if right else 2 * s
            ref = self.buf.at[self.y, zz, self.c, :, self.b]
            local_wait(ref, self.sem.at[self.rb(right, s)])
            if s < 3 or (s == 3 and right):
                self.send(ref, self.zdev(1 if right else -1), 2, self.rb(right, s + 1))
            self.send(ref, self.ydev(1), 3, self.ry(True, k))
            self.send(ref, self.ydev(-1), 3, self.ry(False, k))
            self.share(ref)

    def y_step(self, k):
        zz = self.zat(self.zoff(k))
        for right in (True, False):
            ref = self.buf.at[self.yat(-1 if right else 1), zz, self.c, :, self.b]
            local_wait(ref, self.sem.at[self.ry(right, k)])
            if (k % 2 == 0) == right:
                self.send(ref, self.ydev(1 if right else -1), 3, 47 if right else 48)
            self.share(ref)

    def far(self):
        for s in (47, 48):
            local_wait(self.buf.at[0, pl.ds(0, 4), self.c, :, self.b], self.sem.at[s])
        self.share(self.buf.at[self.yat(2), :, self.c, :, self.b])

    def finish(self):
        local_wait(self.buf.at[:, :, 1 - self.c, :, pl.ds(0, COLS)], self.sem.at[5])

    def drain(self):
        local_wait(self.buf.at[pl.ds(0, 3), 0, 0, :, self.a], self.sem.at[0])
        local_wait(self.buf.at[:, pl.ds(0, 7), 0, :, self.a], self.sem.at[1])
        local_wait(self.buf.at[0, pl.ds(0, 7), 0, :, self.b], self.sem.at[2])
        local_wait(self.buf.at[pl.ds(0, 3), :, 0, :, self.b], self.sem.at[3])
        local_wait(self.buf.at[:, :, self.c, :, pl.ds(0, COLS)], self.sem.at[4])


CUT = 512
SLAB = 16


def remote(src, dst, ssem, rsem, to):
    pltpu.make_async_remote_copy(
        src_ref=src, dst_ref=dst, send_sem=ssem, recv_sem=rsem, device_id=to, device_id_type=MESH
    ).start()


def forward_kernel(
    ids_h, tok_h, wk_h, wv_h, wo_h, tgt_h, wq_h, ql_h, qr_h, ol_h, or_h, cos_h, sin_h,
    grad_q, grad_o, fit,
    tok, wk, wv, tgt, wq, ql, qr, ol, orr, cos, sin,
    slab_in, slab_out, left_in, left_out, fac, fac_all, lft, ev,
    ids, wbuf, bt, mt, k4, v4, fb, lft_m, acc, low, part, total,
    sem_l, sem_w, sem_s, sem_t, sem_k, sem_1, sem_2, sem_3, sem_4, sem_f, sem_e, sem_g,
):
    me = place()
    x, z, c, y = me
    p = (x * NZ + z) * NC + c
    f32, bf16 = jnp.float32, jnp.bfloat16
    tokens_n = tok.shape[0]
    half = HEAD_DIM // 2
    sibling = (x, z, 1 - c, y)

    loads = {}
    for i, (name, src, dst) in enumerate(
        (
            ("wq", wq_h, wq),
            ("ql", ql_h, ql),
            ("or", or_h, orr),
            ("qr", qr_h, qr),
            ("ol", ol_h, ol),
            ("wo", wo_h, wbuf.at[y, z, c, :, pl.ds(0, COLS)]),
            ("tok", tok_h, tok),
            ("wk", wk_h, wk),
            ("wv", wv_h, wv),
            ("cos", cos_h, cos),
            ("sin", sin_h, sin),
            ("tgt", tgt_h, tgt),
            ("ids", ids_h, ids),
        )
    ):
        loads[name] = pltpu.make_async_copy(src, dst, sem_l.at[i])
        loads[name].start()

    barrier = pltpu.get_barrier_semaphore()

    def greet(to):
        pl.semaphore_signal(barrier, inc=1, device_id=to, device_id_type=MESH)

    for dx, dz, dc in PEERS:
        greet(((x + dx) % NX, (z + dz) % NZ, (c + dc) % NC, y))

    for dy, dz, dc in PEERS:
        if dy:
            greet((x, (z + dz) % NZ, (c + dc) % NC, (y + dy) % NY))

    for dx in range(1, NX):
        for dy in range(1, NY):
            greet(((x + dx) % NX, z, c, (y + dy) % NY))

    def turned(v):
        first, second = v[:half], v[half:]
        ct, st = cos[...], sin[...]
        return jnp.concatenate([first * ct - second * st, second * ct + first * st], axis=0)

    for name in ("ids", "wq", "ql", "or", "qr", "ol"):
        loads[name].wait()
    sign = (1 - 2 * (ids[...].reshape(1, 1) % 2)).astype(f32)
    slabs = wq[...].astype(f32).T.reshape(COLS // SLAB, 2, 8, ROWS).astype(bf16)
    for i in range(2):
        slab_in[pl.ds(0, COLS // SLAB), :, pl.ds(i * ROWS, ROWS)] = slabs[:, i]
    slab_in[pl.ds(COLS // SLAB, PLANE - COLS // SLAB)] = jnp.zeros(
        (PLANE - COLS // SLAB, 8, 128), bf16
    )
    fac[...] = jnp.concatenate([qr[...].astype(f32), ol[...].astype(f32)], axis=0).astype(bf16)
    lft[...] = (jnp.concatenate([ql[...].astype(f32), orr[...].astype(f32)], axis=0) * sign).astype(bf16)
    fb[:, :, pl.ds(COLS, 128)] = jnp.zeros((NY, 8, 128), bf16)
    slab_out[p] = slab_in[p]
    fac_all[x * NZ + z, c] = fac[...]

    loads["wo"].wait()
    loads["tgt"].wait()
    pl.semaphore_wait(barrier, PLANE - 1 + 3 * NZ * NC + 9)

    def to_plane(src, dst, sem):
        for dx, dz, dc in PEERS:
            xx, zz, cc = (x + dx) % NX, (z + dz) % NZ, (c + dc) % NC
            remote(src.at[(xx * NZ + zz) * NC + cc], dst.at[p], sem.at[0], sem.at[1], (xx, zz, cc, y))

    to_plane(slab_in, slab_out, sem_s)

    @pl.when(x != y)
    def _():
        remote(lft, lft_m, sem_t.at[0], sem_t.at[1], (y, z, c, x))

    wide = PlaneGather(me, wbuf, sem_w, CUT)
    wide.start()

    @pl.when(x == y)
    def _():
        lft_m[...] = lft[...]

    for name in ("tok", "wk", "wv", "cos", "sin"):
        loads[name].wait()
    key_t = jnp.dot(tok[...], wk[...], preferred_element_type=f32).T
    k4[y] = turned(key_t).T.astype(bf16)
    v4[y] = jnp.dot(tok[...], wv[...], preferred_element_type=f32).T.astype(bf16)
    key_half = k4.at[y, pl.ds(pl.multiple_of(c * 128, 128), 128)]
    value_half = v4.at[y, pl.ds(pl.multiple_of(c * 64, 64), 64)]
    for d in range(1, NY):
        to = (x, z, c, (y + d) % NY)
        remote(key_half, key_half, sem_k.at[0], sem_k.at[1], to)
        remote(value_half, value_half, sem_k.at[2], sem_k.at[3], to)

    for i in range(PLANE):
        left_in[i, :, pl.ds(0, ROWS)] = lft[:, pl.ds(i * ROWS, ROWS)]
    left_out[p] = left_in[p]

    @pl.when(x != y)
    def _():
        local_wait(lft_m, sem_t.at[1])

    out_right = lft_m[pl.ds(RANK, RANK), pl.ds(pl.multiple_of(x * COLS, 128), COLS)].astype(f32)
    beside = jnp.concatenate([out_right] * 3 + [jnp.zeros((128 - 3 * RANK, COLS), f32)], axis=0)
    beside = beside.T.astype(bf16).reshape(NZ, NC, ROWS, 128)
    for b in range(NY):
        wbuf[b, :, :, :, pl.ds(COLS, 128)] = beside

    local_wait(slab_out.at[pl.ds(0, PLANE - 1)], sem_s.at[1])
    made = lax.dot_general(
        jnp.concatenate(
            [
                jnp.concatenate(
                    [slab_out[i, :, pl.ds(h * ROWS, ROWS)] for i in range(PLANE)], axis=1
                )
                for h in range(2)
            ]
            + [lft_m[...]],
            axis=0,
        ),
        tok[...],
        (((1,), (1,)), ((), ())),
        preferred_element_type=f32,
    )
    bt[y, x, z, c] = made[:SLAB].astype(bf16)
    low[...] = made[SLAB : SLAB + 8].astype(bf16)
    mine = bt.at[y, x, z, c]
    for d in (4, 3, 5, 2, 6, 1, 7):
        remote(mine, mine, sem_1.at[0], sem_1.at[1], (x, (z + d) % NZ, c, y))

    wide.a_line()
    wide.b_step(1)
    wide.y_step(0)

    local_wait(bt.at[y, x, pl.ds(0, 7), c], sem_1.at[1])

    def line_out(yy):
        ref = bt.at[yy, x, :, c]
        for d in (1, 3, 2):
            remote(ref, ref, sem_3.at[0], sem_3.at[d], ((x + d) % NX, z, c, y))
        remote(ref, ref, sem_4.at[0], sem_4.at[1], sibling)

    line = bt.at[y, x, :, c]
    for d in (2, 1, 3):
        remote(line, line, sem_2.at[0], sem_2.at[d], (x, z, c, (y + d) % NY))
    line_out(y)

    spot = fb.at[y, :, pl.ds(0, COLS)]

    @pl.when(x != y)
    def _():
        remote(fac, spot, sem_t.at[4], sem_t.at[5], (x, z, c, x))

    for d in range(1, NX):
        remote(fac, spot, sem_t.at[4], sem_t.at[5], ((x + d) % NX, z, c, x))

    @pl.when(x == y)
    def _():
        fb[y, :, pl.ds(0, COLS)] = fac[...]

    local_wait(k4.at[pl.ds(0, 3), pl.ds(0, 128)], sem_k.at[1])
    for d in range(1, NY):
        keys_in = k4.at[(y + d) % NY, pl.ds(pl.multiple_of(c * 128, 128), 128)]
        remote(keys_in, keys_in, sem_k.at[4], sem_k.at[5], sibling)
    local_wait(v4.at[pl.ds(0, 3), pl.ds(0, 64)], sem_k.at[3])
    for d in range(1, NY):
        values_in = v4.at[(y + d) % NY, pl.ds(pl.multiple_of(c * 64, 64), 64)]
        remote(values_in, values_in, sem_k.at[7], sem_k.at[6], sibling)
    for d in (1, 3, 2):
        yy = (y + NY - d) % NY
        local_wait(bt.at[yy, x, :, c], sem_2.at[d])
        line_out(yy)

    wide.a_step(1)
    wide.b_step(2)
    wide.y_step(1)
    wide.y_step(2)

    tgt_half = tgt.at[pl.ds(pl.multiple_of(c * 128, 128), 128)]

    @pl.when(x == y)
    def _():
        for d in (2, 1, 3):
            to = (x, z, c, (y + d) % NY)
            remote(tgt_half, tgt_half, sem_t.at[2], sem_t.at[3], to)

    row = lax.broadcasted_iota(jnp.int32, (tokens_n, tokens_n), 0)
    col = lax.broadcasted_iota(jnp.int32, (tokens_n, tokens_n), 1)

    to_log2 = HEAD_DIM ** (-0.5) * math.log2(math.e)

    def attend(xb):
        @pl.loop(0, NY, step=2)
        def _(pair):
            for yh in (pair, pair + 1):
                right = fb[yh, pl.ds(0, RANK), pl.ds(pl.multiple_of(xb * 256, 256), 256)]
                shift = lax.dot_general(
                    right, low[pl.ds(0, RANK), :], (((0,), (0,)), ((), ())), preferred_element_type=f32
                )
                base = bt[yh, xb].reshape(2 * HEAD_DIM, tokens_n).astype(f32)
                query = base + noise_scale * shift
                for j in range(2):
                    q = turned(query[j * HEAD_DIM : (j + 1) * HEAD_DIM]).astype(bf16)
                    scores = jnp.dot(k4[yh], q, preferred_element_type=f32)
                    scores = jnp.where(row <= col, scores, -1e30)
                    scores = jnp.exp2((scores - jnp.max(scores, axis=0, keepdims=True)) * to_log2)
                    share = 1.0 / jnp.sum(scores, axis=0, keepdims=True)
                    mixed = jnp.dot(v4[yh], (scores * share).astype(bf16), preferred_element_type=f32)
                    mt[yh, xb * 2 + j] = mixed.astype(bf16)

    local_wait(bt.at[:, x, :, 1 - c], sem_4.at[1])
    local_wait(k4.at[pl.ds(0, 3), pl.ds(0, 128)], sem_k.at[5])
    local_wait(v4.at[pl.ds(0, 3), pl.ds(0, 64)], sem_k.at[6])

    @pl.when(x != y)
    def _():
        local_wait(fb.at[:, :, pl.ds(0, COLS)], sem_t.at[5])

    @pl.when(x == y)
    def _():
        local_wait(fb.at[pl.ds(0, 3), :, pl.ds(0, COLS)], sem_t.at[5])

    attend(x)
    wide.a_step(2)
    wide.b_step(3)
    wide.y_step(3)
    wide.y_step(4)

    chip = x * NZ + z
    for d in range(1, NZ):
        remote(fac, fac_all.at[chip, c], sem_f.at[0], sem_f.at[1], (x, (z + d) % NZ, c, y))


    def block_in(d):
        ref = bt.at[:, (x + NX - d) % NX, :, c]
        local_wait(ref, sem_3.at[d])
        remote(ref, ref, sem_4.at[0], sem_4.at[1 + d], sibling)

    def block_use(d):
        xb = (x + NX - d) % NX
        local_wait(bt.at[:, xb, :, 1 - c], sem_4.at[1 + d])
        attend(xb)

    block_in(1)
    block_in(3)

    block_use(1)
    wide.a_step(3)
    wide.b_step(4)
    wide.y_step(5)
    wide.y_step(6)
    block_in(2)
    block_use(3)
    wide.a_step(4)
    wide.y_step(7)

    to_plane(left_in, left_out, sem_g)

    @pl.when(x != y)
    def _():
        local_wait(tgt_half, sem_t.at[3])
        remote(tgt_half, tgt_half, sem_t.at[6], sem_t.at[7], sibling)

    block_use(2)
    wide.far()
    local_wait(fac_all.at[pl.ds(0, NZ - 1), c], sem_f.at[1])
    facs = fac_all.at[pl.ds(x * NZ, NZ), c]
    for d in range(1, NX):
        remote(facs, facs, sem_f.at[2], sem_f.at[3], ((x + d) % NX, z, c, y))

    @pl.when(x != y)
    def _():
        local_wait(tgt.at[pl.ds(0, 128)], sem_t.at[7])

    wide.finish()
    acc[...] = -tgt[...].astype(f32).T

    @pl.loop(0, NY)
    def _(b):
        rows = mt[b, pl.ds(0, 7)].reshape(COLS, tokens_n)
        low_o = noise_scale * jnp.dot(
            fb[b, pl.ds(RANK, RANK), pl.ds(0, COLS)], rows, preferred_element_type=f32
        )
        first = low_o.astype(bf16).astype(f32)
        second = (low_o - first).astype(bf16).astype(f32)
        third = low_o - first - second
        low_parts = jnp.concatenate(
            [first, second, third, jnp.zeros((128 - 3 * RANK, tokens_n), f32)], axis=0
        ).astype(bf16)
        term = jnp.dot(
            wbuf[b].reshape(COLS, COLS + 128),
            jnp.concatenate([rows, low_parts], axis=0),
            preferred_element_type=f32,
        )
        acc[...] += term.astype(bf16).astype(f32)

    part[x] = jnp.full((1, 128), jnp.sum(acc[...] * acc[...]), f32)
    for d in range(1, NX):
        remote(part.at[x], part.at[x], sem_e.at[0], sem_e.at[1], ((x + d) % NX, z, c, y))
    local_wait(part.at[pl.ds(0, NX - 1)], sem_e.at[1])
    total[...] = part[0] + part[1] + part[2] + part[3]
    slot = (y * NZ + z) * NC + c
    ev[slot] = total[...]

    for dy, dz, dc in PEERS:
        to = (x, (z + dz) % NZ, (c + dc) % NC, (y + dy) % NY)
        remote(total, ev.at[slot], sem_e.at[2], sem_e.at[3], to)

    local_wait(fac_all.at[pl.ds(0, 3 * NZ), c], sem_f.at[3])
    remote(fac_all.at[:, c], fac_all.at[:, c], sem_f.at[4], sem_f.at[5], sibling)
    local_wait(left_out.at[pl.ds(0, PLANE - 1)], sem_g.at[1])
    local_wait(fac_all.at[:, 1 - c], sem_f.at[5])
    local_wait(ev.at[pl.ds(0, PLANE - 1)], sem_e.at[3])

    scored = -(ev[...].reshape(PLANE, 128) / (tokens_n * D))
    mean = jnp.sum(scored, axis=0, keepdims=True) / PLANE
    apart = scored - mean
    spread = jnp.sum(apart * apart, axis=0, keepdims=True) / PLANE
    weight = apart / jnp.sqrt(spread + spread_floor) / noise_scale
    fit[...] = -(ev[p] / (tokens_n * D))
    rank_at = lax.broadcasted_iota(jnp.int32, (PLANE, 8, 128), 1)
    left = left_out[...].astype(f32) * weight[:, None, :]
    left = jnp.concatenate(
        [
            jnp.where(rank_at < RANK, left, 0.0).reshape(PLANE * 8, 128),
            jnp.where(rank_at < RANK, 0.0, left).reshape(PLANE * 8, 128),
        ],
        axis=1,
    )
    right = fac_all[...].reshape(PLANE * 8, COLS)
    first = left.astype(bf16)
    rest = left - first.astype(f32)
    second = rest.astype(bf16)
    third = (rest - second.astype(f32)).astype(bf16)
    grads = jnp.zeros((256, COLS), f32)
    for piece in (third, second, first):
        grads += lax.dot_general(
            piece, right, (((0,), (0,)), ((), ())), preferred_element_type=f32
        )
    grad_q[...] = grads[:ROWS]
    grad_o[...] = grads[128 : 128 + ROWS]

    wide.drain()
    local_wait(slab_out.at[pl.ds(0, PLANE - 1)], sem_s.at[0])
    local_wait(left_out.at[pl.ds(0, PLANE - 1)], sem_g.at[0])

    @pl.when(x != y)
    def _():
        local_wait(lft_m, sem_t.at[0])
        local_wait(tgt.at[pl.ds(0, 128)], sem_t.at[6])
        local_wait(fb.at[:, :, pl.ds(0, COLS)], sem_t.at[4])

    @pl.when(x == y)
    def _():
        local_wait(tok.at[pl.ds(0, 3 * 128 * COLS // D)], sem_t.at[2])
        local_wait(fb.at[pl.ds(0, 3), :, pl.ds(0, COLS)], sem_t.at[4])

    local_wait(k4.at[pl.ds(0, 3), pl.ds(0, 128)], sem_k.at[0])
    local_wait(v4.at[pl.ds(0, 3), pl.ds(0, 64)], sem_k.at[2])
    local_wait(k4.at[pl.ds(0, 3), pl.ds(0, 128)], sem_k.at[4])
    local_wait(v4.at[pl.ds(0, 3), pl.ds(0, 64)], sem_k.at[7])
    local_wait(bt.at[0, 0, pl.ds(0, 7), 0], sem_1.at[0])
    local_wait(bt.at[pl.ds(0, 3), 0, :, 0], sem_2.at[0])
    local_wait(bt.at[:, pl.ds(0, 3), :, 0], sem_3.at[0])
    local_wait(bt.at[:, :, :, 0], sem_4.at[0])
    local_wait(fac_all.at[pl.ds(0, NZ - 1), c], sem_f.at[0])
    local_wait(fac_all.at[pl.ds(0, 3 * NZ), c], sem_f.at[2])
    local_wait(fac_all.at[:, c], sem_f.at[4])
    local_wait(part.at[pl.ds(0, NX - 1)], sem_e.at[0])
    local_wait(ev.at[pl.ds(0, PLANE - 1)], sem_e.at[2])


def forward(ids, *ins):
    tok = ins[0].shape[0]
    bf16, f32 = jnp.bfloat16, jnp.float32
    held = [a for i, a in enumerate(ins) if i not in (3,)]
    order = (0, 1, 2, 3, 4, 5, 6, 7, 8, 9, 10)
    dma = pltpu.SemaphoreType.DMA
    return pl.pallas_call(
        forward_kernel,
        name="forward",
        out_shape=(
            jax.ShapeDtypeStruct((ROWS, COLS), f32),
            jax.ShapeDtypeStruct((ROWS, COLS), f32),
            jax.ShapeDtypeStruct((1, 128), f32),
        ),
        in_specs=[pl.BlockSpec(memory_space=pl.ANY)] * (1 + len(ins)),
        out_specs=[pl.BlockSpec(memory_space=pltpu.VMEM)] * 3,
        scratch_shapes=[pltpu.VMEM(held[i].shape, held[i].dtype) for i in order]
        + [
            pltpu.VMEM((PLANE, 8, 128), bf16),
            pltpu.VMEM((PLANE, 8, 128), bf16),
            pltpu.VMEM((PLANE, 8, 128), bf16),
            pltpu.VMEM((PLANE, 8, 128), bf16),
            pltpu.VMEM((8, COLS), bf16),
            pltpu.VMEM((NX * NZ, NC, 8, COLS), bf16),
            pltpu.VMEM((8, D), bf16),
            pltpu.VMEM((PLANE, 1, 128), f32),
            pltpu.VMEM((1,), jnp.int32),
            pltpu.VMEM((NY, NZ, NC, ROWS, COLS + 128), bf16),
            pltpu.VMEM((NY, NX, NZ, NC, SLAB, tok), bf16),
            pltpu.VMEM((NY, 8, HEAD_DIM, tok), bf16),
            pltpu.VMEM((NY, tok, HEAD_DIM), bf16),
            pltpu.VMEM((NY, HEAD_DIM, tok), bf16),
            pltpu.VMEM((NY, 8, COLS + 128), bf16),
            pltpu.VMEM((8, D), bf16),
            pltpu.VMEM((COLS, tok), f32),
            pltpu.VMEM((8, tok), bf16),
            pltpu.VMEM((NX, 1, 128), f32),
            pltpu.VMEM((1, 128), f32),
            dma((13,)),
            dma((PlaneGather.SEMS,)),
            dma((2,)),
            dma((8,)),
            dma((8,)),
            dma((2,)),
            dma((4,)),
            dma((4,)),
            dma((5,)),
            dma((6,)),
            dma((4,)),
            dma((2,)),
        ],
        compiler_params=pltpu.CompilerParams(
            collective_id=0, has_side_effects=True, vmem_limit_bytes=60 * 1024 * 1024
        ),
    )(ids, *ins)


def hand_on(*arrays):
    def body(*refs):
        for i in range(len(arrays)):
            refs[len(arrays) + i][...] = refs[i][...]

    return pl.pallas_call(
        body,
        name="hand_on",
        out_shape=[jax.ShapeDtypeStruct(a.shape, a.dtype) for a in arrays],
        in_specs=[pl.BlockSpec(memory_space=pltpu.VMEM)] * len(arrays),
        out_specs=[pl.BlockSpec(memory_space=pltpu.VMEM)] * len(arrays),
    )(*arrays)


def tables(count, head_size):
    position = np.arange(count, dtype=np.float64)
    index = np.arange(head_size // 2, dtype=np.float64)
    freq = np.exp(-math.log(rope_base) * 2.0 * index / head_size)
    angle = freq[:, None] * position[None, :]
    return np.cos(angle).astype(np.float32), np.sin(angle).astype(np.float32)


def per_device(
    tokens,
    target,
    w_query,
    w_key,
    w_value,
    w_out,
    query_left_factors,
    query_right_factors,
    o_left,
    o_right,
    member_ids,
):
    cos_t, sin_t = tables(tokens.shape[0], HEAD_DIM)
    grad_q, grad_o, fit = forward(
        member_ids,
        tokens,
        w_key,
        w_value,
        jnp.transpose(w_out),
        target,
        w_query,
        jnp.transpose(query_left_factors[0]),
        query_right_factors[0],
        jnp.transpose(o_left[0]),
        o_right[0],
        cos_t,
        sin_t,
    )
    grad_q, grad_o, fit = hand_on(grad_q, grad_o, fit)
    return (grad_q, jnp.transpose(grad_o), fit[0, :1])


def solution(mesh):
    torus = Mesh(mesh.devices.reshape(NX, NZ, NC, NY), AXES)
    placed = (
        P(),
        P(None, "mp"),
        P(POP, "mp"),
        P(None, "mp"),
        P(None, "mp"),
        P("mp", POP),
        P(POP, None, None),
        P(POP, None, "mp"),
        P(POP, "mp", None),
        P(POP, None, None),
        P(POP),
    )
    return jax.shard_map(
        per_device,
        mesh=torus,
        in_specs=placed,
        out_specs=(P(POP, "mp"), P("mp", POP), P(POP)),
        check_vma=False,
    )
```
